32 devices in a mesh: blk: 16 (over z, y, core), tp: 2 (over x).
Axes of the slice: x: 2, y: 2, z: 4, core: 2. Of those that a mesh axis runs over, the one named last changes fastest.
Arguments:
- dec_states: bfloat16 [4096, 5120], P('blk', 'tp'), may hold values from -200 to 200
- norm_gain: float32 [5120], replicated, may hold values from 0.1 to 1.9
- query_weight: bfloat16 [5120, 768], P(None, 'tp'), may hold values from -0.078125 to 0.078125
- out_weight: bfloat16 [768, 5120], P('tp'), may hold values from -0.21875 to 0.21875
- enc_keys: bfloat16 [6144, 768], P('blk', 'tp'), may hold values from -1000 to 1000
- enc_values: bfloat16 [6144, 768], P('blk', 'tp'), may hold values from -6 to 6
Outputs:
- attn_out: bfloat16 [4096, 5120], P('blk', 'tp')
The draws below stay inside these ranges and needn't reach their ends.
All inputs are finite; a program needn't handle non-finite values.
Results may differ from the reference program's by a relative error of at most 0.034.
Values may be sent and summed in bfloat16 or wider, within the bound.
A program may use at most 128 MiB of HBM per device.

```python
import math
import jax
import jax.numpy as jnp
from jax import lax

D = 5120
HEAD_DIM = 128
Q_DEV = 256
HEADS = 6
DEC_TOK = 4096
ENC_TOK = 6144


def draw_dec_states(key, part):
    key_base, key_rows, key_cols = jax.random.split(key, 3)
    base = jnp.clip(jax.random.normal(key_base, (DEC_TOK, D), jnp.float32), -6.0, 6.0)
    row_scale = jnp.exp(jax.random.uniform(key_rows, (DEC_TOK, 1), jnp.float32) * jnp.log(10.0))
    ramp = 1.0 + 2.0 * jnp.arange(D, dtype=jnp.float32) / D
    col_scale = jnp.exp(jax.random.uniform(key_cols, (1, D), jnp.float32) * jnp.log(10.0)) * ramp[None, :]
    return (base * row_scale * col_scale / 10.0).astype(jnp.bfloat16)


def draw_enc_keys(key, part):
    key_base = jax.random.fold_in(key, 0)
    base = jnp.clip(jax.random.normal(key_base, (ENC_TOK, HEADS * HEAD_DIM), jnp.float32), -6.0, 6.0)
    return base.astype(jnp.bfloat16)


def shard_levels(key, shape, cuts, low, top_value):
    gain = 1.0
    for dim, parts in cuts:
        draws = jax.random.uniform(jax.random.fold_in(jax.random.fold_in(key, 6), dim), (parts,), jnp.float32, low / len(cuts), top_value / len(cuts))
        gain = gain * jnp.repeat(jnp.exp(draws), shape[dim] // parts).reshape((-1,) + (1,) * (len(shape) - 1 - dim))
    return gain


def noise(rng, extent, width, most, pieces=(), kind=jnp.bfloat16):
    values = jax.random.normal(rng, extent, jnp.float32) * width
    if len(pieces) > 0:
        values = shard_levels(rng, extent, pieces, -0.22, 0.18) * values
    return jnp.clip(values, min=-most, max=most).astype(kind)


def setup_inputs(seed: int = 0) -> dict:
    arg_keys = jax.random.split(jax.random.key(seed), 7)
    dec_states = draw_dec_states(jax.random.fold_in(arg_keys[6], 71), 0)
    norm_gain = jnp.clip(1.0 + 0.18 * jax.random.normal(arg_keys[1], (D,), jnp.float32), 0.1, 1.9)
    query_weight = noise(arg_keys[2], (D, HEADS * HEAD_DIM), D ** -0.5, 0.078125, ((1, 2),))
    out_weight = noise(arg_keys[3], (HEADS * HEAD_DIM, D), (HEADS * HEAD_DIM) ** -0.5, 0.21875, ((0, 2),))
    enc_keys = draw_enc_keys(jax.random.fold_in(arg_keys[6], 71), 0)
    enc_values = noise(arg_keys[5], (ENC_TOK, HEADS * HEAD_DIM), 1.0, 6.0, ((0, 16), (1, 2)))
    return {"dec_states": dec_states, "norm_gain": norm_gain, "query_weight": query_weight, "out_weight": out_weight, "enc_keys": enc_keys, "enc_values": enc_values}


NORM_EPS = 1e-06

def reference(dec_states, norm_gain, query_weight, out_weight, enc_keys, enc_values):
    states = dec_states.astype(jnp.float32)
    mean_sq = lax.optimization_barrier(jnp.mean(states * states, axis=1, keepdims=True))
    normed = (states * lax.rsqrt(mean_sq + NORM_EPS) * norm_gain.astype(jnp.float32)).astype(jnp.bfloat16)
    queries = jnp.dot(normed, query_weight, preferred_element_type=jnp.float32).astype(jnp.bfloat16)
    query_heads = queries.reshape(DEC_TOK // Q_DEV, Q_DEV, HEADS, HEAD_DIM).transpose(2, 0, 1, 3)
    key_heads = enc_keys.reshape(ENC_TOK, HEADS, HEAD_DIM).transpose(1, 0, 2)
    value_heads = enc_values.reshape(ENC_TOK, HEADS, HEAD_DIM).transpose(1, 0, 2)
    score_scale = 1.0 / math.sqrt(HEAD_DIM)

    def one_head(operands):
        query_blocks, key_rows, value_rows = operands

        def one_block(query_rows):
            scores = jnp.dot(query_rows, key_rows.T, preferred_element_type=jnp.float32) * score_scale
            row_peak = lax.optimization_barrier(jnp.max(scores, axis=1, keepdims=True))
            exp_scores = jnp.exp(scores - row_peak)
            row_total = lax.optimization_barrier(jnp.sum(exp_scores, axis=1, keepdims=True))
            mixed = jnp.dot(exp_scores.astype(jnp.bfloat16), value_rows, preferred_element_type=jnp.float32)
            return mixed / row_total
        return lax.map(one_block, query_blocks)
    attended = lax.map(one_head, (query_heads, key_heads, value_heads))
    attended = attended.transpose(1, 2, 0, 3).reshape(DEC_TOK, HEADS * HEAD_DIM).astype(jnp.bfloat16)
    return jnp.dot(attended, out_weight, preferred_element_type=jnp.float32).astype(jnp.bfloat16)
```

```python
import functools
import math

import jax
import jax.numpy as jnp
from jax import lax
from jax.experimental import pallas as pl
from jax.experimental.pallas import tpu as pltpu
from jax.sharding import PartitionSpec as P

HEAD_DIM = 128
NORM_EPS = 1e-06
LANES = 128
SUBS = 2


def column_tile(width, limit=640):
    best = LANES
    for tile in range(LANES, limit + 1, LANES):
        if width % tile == 0:
            best = tile
    return best


def kernel(
    n_blk,
    n_tp,
    x_hbm,
    gain_ref,
    wq_hbm,
    wo_hbm,
    k_hbm,
    v_hbm,
    out_hbm,
    kvbuf,
    wq_own,
    wq,
    wo,
    xbuf,
    xg,
    qsend,
    qrecv,
    own_part,
    sqbuf,
    fbuf,
    qbuf,
    qmate,
    osend,
    orecv,
    ssend,
    srecv,
    opart,
    lse_own,
    att,
    oacc,
    obuf,
    kv_send,
    kv_recv,
    wq_send,
    wq_recv,
    wo_send,
    wo_recv,
    sq_send,
    sq_recv,
    head_send,
    head_recv,
    mate_send,
    mate_recv,
    kv_local,
    local_sem,
    out_sem,
):
    n_line = n_blk // 4
    n_pair = n_line // 2
    b = lax.axis_index("blk")
    t = lax.axis_index("tp")
    core = lax.rem(b, 2)
    side = lax.rem(lax.div(b, 2), 2)
    line = lax.div(b, 4)
    par = lax.rem(line, 2)
    pair = lax.div(line, 2)
    rows = x_hbm.shape[0]
    feat = x_hbm.shape[1]
    width = wq_hbm.shape[1]
    heads = width // HEAD_DIM
    span = n_tp * HEAD_DIM
    last = heads - 1
    wq_rows = feat // (4 * SUBS)
    wo_rows = HEAD_DIM // 4

    def index(zz, yy, cc):
        return (zz * 2 + yy) * 2 + cc

    sibling = index(line, side, 1 - core)
    beside = index(line, 1 - side, core)
    partner = index(line + 1 - 2 * par, side, core)
    peers = [lax.rem(t + off, n_tp) for off in range(1, n_tp)]
    mates = [lax.rem(pair + off, n_pair) for off in range(1, n_pair)]

    def mate_index(m):
        return index(2 * m + par, side, core)

    def ds(start, size, mult=LANES):
        return pl.ds(pl.multiple_of(start, mult), size)

    def head_cols(h):
        return slice(h * HEAD_DIM, (h + 1) * HEAD_DIM)

    def slot(pp, yy, cc):
        return (pp * 2 + yy) * 2 + cc

    mine = slot(par, side, core)

    kv_loads = [
        pltpu.make_async_copy(
            (k_hbm, v_hbm)[e % 2].at[:, head_cols(e // 2)], kvbuf.at[e, mine], kv_local.at[e]
        )
        for e in range(2 * heads)
    ]
    x_load = pltpu.make_async_copy(x_hbm, xbuf, local_sem.at[0])
    wq_load = pltpu.make_async_copy(wq_hbm.at[ds(t * feat, feat)], wq_own, local_sem.at[1])
    wo_loads = [
        pltpu.make_async_copy(
            wo_hbm.at[head_cols(h), ds(t * feat, feat)],
            wo.at[ds(h * span + t * HEAD_DIM, HEAD_DIM)],
            local_sem.at[2 + h],
        )
        for h in range(heads)
    ]
    for load in kv_loads[:2] + [x_load, wq_load] + kv_loads[2:] + wo_loads:
        load.start()

    barrier = pltpu.get_barrier_semaphore()
    for other in [sibling, beside, partner] + [mate_index(m) for m in mates]:
        pl.semaphore_signal(barrier, inc=1, device_id={"blk": other})
    for p in peers:
        pl.semaphore_signal(barrier, inc=1, device_id={"tp": p})
    pl.semaphore_wait(barrier, 3 + len(mates) + len(peers))

    sends = []

    def remote(src, dst, send_sem, recv_sem, device_id):
        return pltpu.make_async_remote_copy(
            src_ref=src, dst_ref=dst, send_sem=send_sem, recv_sem=recv_sem, device_id=device_id
        )

    def launch(copy):
        copy.start()
        sends.append(copy)

    def kv_copy(e, s, k, target):
        ref = kvbuf.at[e, s]
        return remote(ref, ref, kv_send.at[e, k], kv_recv.at[e, s], {"blk": target})

    def kv_wait(e, s):
        kv_copy(e, s, 0, sibling).wait_recv()

    from_beside = slot(par, 1 - side, core)
    from_partner = slot(1 - par, side, core)
    from_corner = slot(1 - par, 1 - side, core)

    def kv_own(h):
        for e in (2 * h, 2 * h + 1):
            kv_loads[e].wait()
            launch(kv_copy(e, mine, 1, partner))
            launch(kv_copy(e, mine, 0, beside))
            launch(kv_copy(e, mine, 3, sibling))

    def kv_pass(h):
        for e in (2 * h, 2 * h + 1):
            kv_wait(e, from_partner)
            launch(kv_copy(e, from_partner, 2, beside))
            launch(kv_copy(e, from_partner, 4, sibling))
            kv_wait(e, from_beside)
            launch(kv_copy(e, from_beside, 5, sibling))

    def kv_corner(h):
        for e in (2 * h, 2 * h + 1):
            kv_wait(e, from_corner)
            launch(kv_copy(e, from_corner, 6, sibling))

    def kv_ready(h):
        for e in (2 * h, 2 * h + 1):
            for pp, yy in ((par, side), (par, 1 - side), (1 - par, side), (1 - par, 1 - side)):
                kv_wait(e, slot(pp, yy, 1 - core))

    def wq_chunk(pp, cc, sub):
        return (pp * 2 + cc) * SUBS + sub

    def wq_ref(p, h, c):
        return wq.at[p, h, ds(c * wq_rows, wq_rows, 16)]

    def wq_hop(p, h, c, k, target):
        ref = wq_ref(p, h, c)
        return remote(ref, ref, wq_send.at[p, h, k], wq_recv.at[p, h, c], {"blk": target})

    def wq_wait(p, h, c):
        wq_hop(p, h, c, 0, sibling).wait_recv()

    def wq_start(h):
        for sub in range(SUBS):
            for p in peers:
                c = wq_chunk(par, core, sub)
                src = wq_hbm.at[ds(p * feat + c * wq_rows, wq_rows, 16), head_cols(h)]
                launch(
                    remote(
                        src, wq_ref(t, h, c), wq_send.at[p, h, sub], wq_recv.at[t, h, c], {"tp": p}
                    )
                )

    def wq_pass(h):
        for sub in range(SUBS):
            for p in peers:
                c = wq_chunk(par, core, sub)
                wq_wait(p, h, c)
                launch(wq_hop(p, h, c, SUBS + sub, partner))
                launch(wq_hop(p, h, c, 2 * SUBS + sub, sibling))

    def wq_relay(h):
        for sub in range(SUBS):
            for p in peers:
                c = wq_chunk(1 - par, core, sub)
                wq_wait(p, h, c)
                launch(wq_hop(p, h, c, 3 * SUBS + sub, sibling))

    def q_copy(p, h, s):
        return remote(
            qsend.at[p, h], qrecv.at[s, h], head_send.at[0, p, h], head_recv.at[0, s, h], {"tp": p}
        )

    def q_part(h):
        for p in peers:
            for pp in (par, 1 - par):
                for sub in range(SUBS):
                    wq_wait(p, h, wq_chunk(pp, 1 - core, sub))
            qsend[p, h] = jnp.dot(
                xg[...], wq[p, h], preferred_element_type=jnp.float32
            ).astype(jnp.bfloat16)
            launch(q_copy(p, h, t))

    def sq_copy(p, s):
        ref = sqbuf.at[s]
        return remote(ref, ref, sq_send.at[p], sq_recv.at[s], {"tp": p})

    tile = column_tile(feat)

    def norm():
        x_load.wait()
        squares = jnp.zeros((rows, 1), jnp.float32)
        for start in range(0, feat, tile):
            piece = xbuf[:, start : start + tile].astype(jnp.float32)
            squares += jnp.sum(piece * piece, axis=1, keepdims=True)
            gain = gain_ref[:, ds(t * feat + start, tile)]
            xg[:, start : start + tile] = (piece * gain).astype(jnp.bfloat16)
        wide = jnp.broadcast_to(squares, (rows, LANES))
        sqbuf[t] = jnp.transpose(wide)[0:8, :]
        for p in peers:
            launch(sq_copy(p, t))
        wq_load.wait()
        own_part[...] = jnp.dot(xg[...], wq_own[...], preferred_element_type=jnp.float32)

    def factor():
        total = sqbuf[t][0:1, :]
        for p in peers:
            sq_copy(p, p).wait_recv()
            total = total + sqbuf[p][0:1, :]
        column = jnp.transpose(jnp.broadcast_to(total, (LANES, rows)))
        scale = math.log2(math.e) / math.sqrt(HEAD_DIM)
        fbuf[...] = lax.rsqrt(column / (feat * n_tp) + NORM_EPS) * scale

    def mate_copy(k, src, dst, h, m, s):
        return remote(
            src, dst, mate_send.at[k, h, m], mate_recv.at[k, h, s], {"blk": mate_index(m)}
        )

    def mq_copy(h, m, s):
        return mate_copy(0, qbuf.at[h], qmate.at[h, s], h, m, s)

    def mo_copy(h, m, s):
        return mate_copy(1, osend.at[h, m], orecv.at[h, s], h, m, s)

    def ms_copy(h, m, s):
        return mate_copy(2, ssend.at[h, m], srecv.at[h, s], h, m, s)

    def q_make(h):
        summed = own_part[:, head_cols(h)]
        for p in peers:
            q_copy(p, h, p).wait_recv()
            summed = summed + qrecv[p, h].astype(jnp.float32)
        qbuf[h] = (summed * fbuf[...]).astype(jnp.bfloat16)
        for m in mates:
            launch(mq_copy(h, m, pair))

    def attend(h, query):
        scores = []
        for i in range(4):
            keys = kvbuf[2 * h, 2 * i : 2 * i + 2].reshape(-1, HEAD_DIM)
            scores.append(
                lax.dot_general(
                    query, keys, (((1,), (1,)), ((), ())), preferred_element_type=jnp.float32
                )
            )
        top = scores[0]
        for s in scores[1:]:
            top = jnp.maximum(top, s)
        top = jnp.max(top, axis=1, keepdims=True)
        mixed = jnp.zeros((rows, 2 * HEAD_DIM), jnp.float32)
        for i in range(4):
            vals = kvbuf[2 * h + 1, 2 * i : 2 * i + 2].reshape(-1, HEAD_DIM)
            wide = jnp.concatenate([vals, jnp.ones_like(vals)], axis=1)
            weights = jnp.exp2(scores[i] - top).astype(jnp.bfloat16)
            mixed = mixed + jnp.dot(weights, wide, preferred_element_type=jnp.float32)
        total = mixed[:, HEAD_DIM:]
        return mixed[:, :HEAD_DIM] / total, top + jnp.log(total) * math.log2(math.e)

    def att_own(h):
        opart[h], lse_own[h] = attend(h, qbuf[h])

    def att_mate(h):
        for m in mates:
            mq_copy(h, m, m).wait_recv()
            out, lse = attend(h, qmate[h, m])
            osend[h, m] = out.astype(jnp.bfloat16)
            launch(mo_copy(h, m, pair))
            ssend[h, m] = jnp.transpose(lse)[0:8, :]
            launch(ms_copy(h, m, pair))

    def att_cols(p, h):
        return att.at[:, ds(h * span + p * HEAD_DIM, HEAD_DIM)]

    def att_copy(p, h, s):
        ref = att_cols(s, h)
        return remote(ref, ref, head_send.at[1, p, h], head_recv.at[1, s, h], {"tp": p})

    def merge(h):
        parts = [opart[h]]
        logs = [lse_own[h]]
        for m in mates:
            mo_copy(h, m, m).wait_recv()
            ms_copy(h, m, m).wait_recv()
            parts.append(orecv[h, m].astype(jnp.float32))
            logs.append(jnp.transpose(jnp.broadcast_to(srecv[h, m][0:1, :], (LANES, rows))))
        top = logs[0]
        for log in logs[1:]:
            top = jnp.maximum(top, log)
        shares = [jnp.exp2(log - top) for log in logs]
        total = shares[0]
        mixed = shares[0] * parts[0]
        for share, part in zip(shares[1:], parts[1:]):
            total = total + share
            mixed = mixed + share * part
        att[:, ds(h * span + t * HEAD_DIM, HEAD_DIM)] = (mixed / total).astype(jnp.bfloat16)
        for p in peers:
            launch(att_copy(p, h, t))

    def wo_ref(p, h, q):
        return wo.at[ds(h * span + p * HEAD_DIM + q * wo_rows, wo_rows, wo_rows)]

    def wo_hop(p, h, q, k, target):
        ref = wo_ref(p, h, q)
        return remote(ref, ref, wo_send.at[p, h, k], wo_recv.at[p, h, q], {"blk": target})

    def wo_wait(p, h, q):
        wo_hop(p, h, q, 0, sibling).wait_recv()

    def wo_start(h):
        q = side * 2 + core
        for p in peers:
            src = wo_hbm.at[ds(h * HEAD_DIM + q * wo_rows, wo_rows, wo_rows), ds(p * feat, feat)]
            launch(
                remote(src, wo_ref(t, h, q), wo_send.at[p, h, 0], wo_recv.at[t, h, q], {"tp": p})
            )

    def wo_pass(h):
        for p in peers:
            q = side * 2 + core
            wo_wait(p, h, q)
            launch(wo_hop(p, h, q, 1, beside))
            launch(wo_hop(p, h, q, 2, sibling))

    def wo_relay(h):
        for p in peers:
            q = (1 - side) * 2 + core
            wo_wait(p, h, q)
            launch(wo_hop(p, h, q, 3, sibling))

    def wo_ready(h):
        wo_loads[h].wait()
        for p in peers:
            for yy in (side, 1 - side):
                wo_wait(p, h, yy * 2 + 1 - core)

    starts = range(0, feat, tile)

    def project_most():
        for h in range(last):
            wo_ready(h)
            for p in peers:
                att_copy(p, h, p).wait_recv()
        for start in starts:
            cols = slice(start, start + tile)
            oacc[:, cols] = jnp.dot(
                att[:, : last * span], wo[: last * span, cols], preferred_element_type=jnp.float32
            )

    events = []

    def at(when, step, *args):
        events.append((when, len(events), step, args))

    for h in range(heads):
        at(2.0 + 0.1 * h, wq_start, h)
        at(2.5 + 6.0 * h, kv_own, h)
        at(6.5 + 3.6 * h, wq_pass, h)
        at(7.0 + 7.0 * h, kv_pass, h)
        at(10.2 + 3.9 * h, wq_relay, h)
        at(11.5 + 6.5 * h, kv_corner, h)
        at(13.0 + 3.6 * h, q_part, h)
        at(16.7 + 3.8 * h, q_make, h)
        at(17.0 + 3.8 * h, kv_ready, h)
        at(17.2 + 3.8 * h, att_own, h)
        at(21.7 + 3.9 * h, att_mate, h)
        at((13.1 if h == 0 else 20.3) + 0.01 * h, wo_start, h)
        at(26.0 + 3.0 * h, wo_pass, h)
        at(32.5 + 0.1 * h, wo_relay, h)
        at(33.0 + 2.0 * h, merge, h)
    at(4.0, norm)
    at(16.0, factor)
    at(36.0, project_most)
    for when, order, step, args in sorted(events, key=lambda event: event[:2]):
        step(*args)

    wo_ready(last)
    for p in peers:
        att_copy(p, last, p).wait_recv()
    stores = []
    for j, start in enumerate(starts):
        cols = slice(start, start + tile)
        result = oacc[:, cols] + jnp.dot(
            att[:, last * span :], wo[last * span :, cols], preferred_element_type=jnp.float32
        )
        obuf[:, cols] = result.astype(jnp.bfloat16)
        store = pltpu.make_async_copy(obuf.at[:, cols], out_hbm.at[:, cols], out_sem.at[j])
        store.start()
        stores.append(store)
    for copy in sends:
        copy.wait_send()
    for store in stores:
        store.wait()


def per_device(n_blk, n_tp, dec_states, norm_gain, query_weight, out_weight, enc_keys, enc_values):
    rows, feat = dec_states.shape
    width = query_weight.shape[1]
    enc_rows = enc_keys.shape[0]
    heads = width // HEAD_DIM
    n_pair = n_blk // 8
    tiles = feat // column_tile(feat)
    bf16, f32 = jnp.bfloat16, jnp.float32
    dma = pltpu.SemaphoreType.DMA
    anywhere = pl.BlockSpec(memory_space=pl.ANY)
    return pl.pallas_call(
        functools.partial(kernel, n_blk, n_tp),
        out_shape=jax.ShapeDtypeStruct((rows, feat), bf16),
        in_specs=[
            anywhere,
            pl.BlockSpec(memory_space=pltpu.VMEM),
            anywhere,
            anywhere,
            anywhere,
            anywhere,
        ],
        out_specs=anywhere,
        scratch_shapes=[
            pltpu.VMEM((2 * heads, 8, enc_rows, HEAD_DIM), bf16),
            pltpu.VMEM((feat, width), bf16),
            pltpu.VMEM((n_tp, heads, feat, HEAD_DIM), bf16),
            pltpu.VMEM((n_tp * width, feat), bf16),
            pltpu.VMEM((rows, feat), bf16),
            pltpu.VMEM((rows, feat), bf16),
            pltpu.VMEM((n_tp, heads, rows, HEAD_DIM), bf16),
            pltpu.VMEM((n_tp, heads, rows, HEAD_DIM), bf16),
            pltpu.VMEM((rows, width), f32),
            pltpu.VMEM((n_tp, 8, rows), f32),
            pltpu.VMEM((rows, LANES), f32),
            pltpu.VMEM((heads, rows, HEAD_DIM), bf16),
            pltpu.VMEM((heads, n_pair, rows, HEAD_DIM), bf16),
            pltpu.VMEM((heads, n_pair, rows, HEAD_DIM), bf16),
            pltpu.VMEM((heads, n_pair, rows, HEAD_DIM), bf16),
            pltpu.VMEM((heads, n_pair, 8, rows), f32),
            pltpu.VMEM((heads, n_pair, 8, rows), f32),
            pltpu.VMEM((heads, rows, HEAD_DIM), f32),
            pltpu.VMEM((heads, rows, LANES), f32),
            pltpu.VMEM((rows, n_tp * width), bf16),
            pltpu.VMEM((rows, feat), f32),
            pltpu.VMEM((rows, feat), bf16),
            dma((2 * heads, 7)),
            dma((2 * heads, 8)),
            dma((n_tp, heads, 4 * SUBS)),
            dma((n_tp, heads, 4 * SUBS)),
            dma((n_tp, heads, 4)),
            dma((n_tp, heads, 4)),
            dma((n_tp,)),
            dma((n_tp,)),
            dma((2, n_tp, heads)),
            dma((2, n_tp, heads)),
            dma((3, heads, n_pair)),
            dma((3, heads, n_pair)),
            dma((2 * heads,)),
            dma((2 + heads,)),
            dma((tiles,)),
        ],
        compiler_params=pltpu.CompilerParams(
            collective_id=0, has_side_effects=True, vmem_limit_bytes=60 * 1024 * 1024
        ),
    )(dec_states, norm_gain.reshape(1, -1), query_weight, out_weight, enc_keys, enc_values)


def solution(mesh):
    in_specs = (P("blk", "tp"), P(), P(None, "tp"), P("tp", None), P("blk", "tp"), P("blk", "tp"))
    out_specs = P("blk", "tp")
    body = functools.partial(per_device, mesh.shape["blk"], mesh.shape["tp"])
    return jax.shard_map(body, mesh=mesh, in_specs=in_specs, out_specs=out_specs, check_vma=False)
```

```python
import functools
import math

import jax
import jax.numpy as jnp
from jax import lax
from jax.experimental import pallas as pl
from jax.experimental.pallas import tpu as pltpu
from jax.sharding import PartitionSpec as P

HEAD_DIM = 128
NORM_EPS = 1e-06
LANES = 128
SUBS = 2


def column_tile(width, limit=640):
    best = LANES
    for tile in range(LANES, limit + 1, LANES):
        if width % tile == 0:
            best = tile
    return best


def kernel(
    n_blk,
    n_tp,
    x_hbm,
    gain_hbm,
    wq_hbm,
    wo_hbm,
    k_hbm,
    v_hbm,
    out_ref,
    gain_ref,
    kvbuf,
    wq_own,
    wq,
    wo,
    xbuf,
    xg,
    qsend,
    qrecv,
    own_part,
    sqbuf,
    fbuf,
    qbuf,
    qmate,
    osend,
    orecv,
    ssend,
    srecv,
    opart,
    lse_own,
    att,
    oacc,
    send_sem,
    kv_recv,
    kv_core_recv,
    wq_recv,
    wq_core_recv,
    wo_recv,
    wo_core_recv,
    sq_recv,
    head_recv,
    mate_recv,
    kv_local,
    local_sem,
):
    n_line = n_blk // 4
    n_pair = n_line // 2
    b = lax.axis_index("blk")
    t = lax.axis_index("tp")
    core = lax.rem(b, 2)
    side = lax.rem(lax.div(b, 2), 2)
    line = lax.div(b, 4)
    par = lax.rem(line, 2)
    pair = lax.div(line, 2)
    rows = x_hbm.shape[0]
    feat = x_hbm.shape[1]
    width = wq_hbm.shape[1]
    heads = width // HEAD_DIM
    span = n_tp * HEAD_DIM
    last = heads - 1
    wq_rows = feat // (4 * SUBS)
    wo_rows = HEAD_DIM // (4 * SUBS)

    def index(zz, yy, cc):
        return (zz * 2 + yy) * 2 + cc

    sibling = index(line, side, 1 - core)
    beside = index(line, 1 - side, core)
    partner = index(line + 1 - 2 * par, side, core)
    peers = [lax.rem(t + off, n_tp) for off in range(1, n_tp)]
    mates = [lax.rem(pair + off, n_pair) for off in range(1, n_pair)]
    n_peer, n_mate = len(peers), len(mates)

    def mate_index(m):
        return index(2 * m + par, side, core)

    def ds(start, size, mult=LANES):
        return pl.ds(pl.multiple_of(start, mult), size)

    def head_cols(h):
        return slice(h * HEAD_DIM, (h + 1) * HEAD_DIM)

    def slot(pp, yy, cc):
        return (pp * 2 + yy) * 2 + cc

    mine = slot(par, side, core)

    kv_loads = [
        pltpu.make_async_copy(
            (k_hbm, v_hbm)[e % 2].at[:, head_cols(e // 2)], kvbuf.at[e, mine], kv_local.at[e // 2]
        )
        for e in range(2 * heads)
    ]
    x_load = pltpu.make_async_copy(x_hbm, xbuf, local_sem.at[0])
    gain_load = pltpu.make_async_copy(gain_hbm, gain_ref, local_sem.at[3])
    wq_load = pltpu.make_async_copy(wq_hbm.at[ds(t * feat, feat)], wq_own, local_sem.at[1])
    wo_loads = [
        pltpu.make_async_copy(
            wo_hbm.at[head_cols(h), ds(t * feat, feat)],
            wo.at[ds(h * span + t * HEAD_DIM, HEAD_DIM)],
            local_sem.at[2],
        )
        for h in range(heads)
    ]
    for load in kv_loads[:2] + [gain_load, x_load, wq_load] + kv_loads[2:] + wo_loads:
        load.start()

    barrier = pltpu.get_barrier_semaphore()
    for other in [sibling, beside, partner] + [mate_index(m) for m in mates]:
        pl.semaphore_signal(barrier, inc=1, device_id={"blk": other})
    for p in peers:
        pl.semaphore_signal(barrier, inc=1, device_id={"tp": p})
    pl.semaphore_wait(barrier, 3 + len(mates) + len(peers))

    def remote(src, dst, kind, recv_sem, device_id):
        return pltpu.make_async_remote_copy(
            src_ref=src,
            dst_ref=dst,
            send_sem=send_sem.at[kind],
            recv_sem=recv_sem,
            device_id=device_id,
        )

    def arrived(ref, recv_sem):
        remote(ref, ref, 0, recv_sem, {"blk": sibling}).wait_recv()

    def sent(ref, kind):
        remote(ref, ref, kind, kv_core_recv.at[0], {"blk": sibling}).wait_send()

    def kv_send(e, s, kind, target):
        ref = kvbuf.at[e, s]
        remote(ref, ref, 0, kv_recv.at[e, kind], {"blk": target}).start()

    def kv_share(e, s):
        ref = kvbuf.at[e, s]
        remote(ref, ref, 0, kv_core_recv.at[e // 2], {"blk": sibling}).start()

    def kv_wait(e, s, kind):
        arrived(kvbuf.at[e, s], kv_recv.at[e, kind])

    from_beside = slot(par, 1 - side, core)
    from_partner = slot(1 - par, side, core)
    from_corner = slot(1 - par, 1 - side, core)

    by_line = (2 * heads - 1,)

    def kv_loaded(h):
        both = kvbuf.at[2 * h : 2 * h + 2, mine]
        pltpu.make_async_copy(both, both, kv_local.at[h]).wait()

    def kv_line(e):
        kv_send(e, mine, 1, partner)

    def kv_side(e):
        kv_send(e, mine, 0, beside)

    def kv_core(e):
        kv_share(e, mine)

    def kv_from_partner(e):
        kv_wait(e, from_partner, 1)
        if e not in by_line:
            kv_send(e, from_partner, 2, beside)
        kv_share(e, from_partner)

    def kv_from_beside(e):
        kv_wait(e, from_beside, 0)
        if e in by_line:
            kv_send(e, from_beside, 2, partner)
        kv_share(e, from_beside)

    def kv_from_corner(e):
        kv_wait(e, from_corner, 2)
        kv_share(e, from_corner)

    def kv_ready(h):
        arrived(kvbuf.at[2 * h : 2 * h + 2, 0:4], kv_core_recv.at[h])

    def wq_chunk(pp, cc, sub):
        return (pp * 2 + cc) * SUBS + sub

    def wq_ref(p, h, c):
        return wq.at[p, h, ds(c * wq_rows, wq_rows, 16)]

    def wq_hop(j, h, c, k):
        ref = wq_ref(peers[j], h, c)
        remote(ref, ref, 1, wq_recv.at[j, h, k], {"blk": partner}).start()

    def wq_share(j, h, c):
        ref = wq_ref(peers[j], h, c)
        remote(ref, ref, 1, wq_core_recv.at[j, h], {"blk": sibling}).start()

    def wq_start(h):
        for k in range(2 * SUBS if h == last else SUBS):
            for j, p in enumerate(peers):
                c = wq_chunk(par if k < SUBS else 1 - par, core, k % SUBS)
                src = wq_hbm.at[ds(p * feat + c * wq_rows, wq_rows, 16), head_cols(h)]
                place = wq_recv.at[n_peer - 1 - j, h, k]
                remote(src, wq_ref(t, h, c), 1, place, {"tp": p}).start()

    def wq_pass(h, sub):
        for j, p in enumerate(peers):
            c = wq_chunk(par, core, sub)
            arrived(wq_ref(p, h, c), wq_recv.at[j, h, sub])
            if h != last:
                wq_hop(j, h, c, SUBS + sub)
            wq_share(j, h, c)

    def wq_relay(h, sub):
        for j, p in enumerate(peers):
            c = wq_chunk(1 - par, core, sub)
            arrived(wq_ref(p, h, c), wq_recv.at[j, h, SUBS + sub])
            wq_share(j, h, c)

    def q_part(h):
        for j, p in enumerate(peers):
            arrived(wq.at[p, h, 0 : feat // 2], wq_core_recv.at[j, h])
            qsend[p, h] = jnp.dot(
                xg[...], wq[p, h], preferred_element_type=jnp.float32
            ).astype(jnp.bfloat16)
            place = head_recv.at[0, n_peer - 1 - j, h]
            remote(qsend.at[p, h], qrecv.at[t, h], 3, place, {"tp": p}).start()

    tile = column_tile(feat)

    def norm():
        gain_load.wait()
        x_load.wait()
        squares = jnp.zeros((rows, 1), jnp.float32)
        for start in range(0, feat, tile):
            piece = xbuf[:, start : start + tile].astype(jnp.float32)
            squares += jnp.sum(piece * piece, axis=1, keepdims=True)
            gain = gain_ref[:, ds(t * feat + start, tile)]
            xg[:, start : start + tile] = (piece * gain).astype(jnp.bfloat16)
        wide = jnp.broadcast_to(squares, (rows, LANES))
        sqbuf[t] = jnp.transpose(wide)[0:8, :]
        for j, p in enumerate(peers):
            ref = sqbuf.at[t]
            remote(ref, ref, 2, sq_recv.at[n_peer - 1 - j], {"tp": p}).start()
        wq_load.wait()
        own_part[...] = jnp.dot(xg[...], wq_own[...], preferred_element_type=jnp.float32)

    def factor():
        total = sqbuf[t][0:1, :]
        for j, p in enumerate(peers):
            arrived(sqbuf.at[p], sq_recv.at[j])
            total = total + sqbuf[p][0:1, :]
        column = jnp.transpose(jnp.broadcast_to(total, (LANES, rows)))
        scale = math.log2(math.e) / math.sqrt(HEAD_DIM)
        fbuf[...] = lax.rsqrt(column / (feat * n_tp) + NORM_EPS) * scale

    def mate_send(k, src, dst, h, i):
        place = mate_recv.at[k, h, n_mate - 1 - i]
        remote(src, dst, 5 + k, place, {"blk": mate_index(mates[i])}).start()

    def q_make(h):
        summed = own_part[:, head_cols(h)]
        for j, p in enumerate(peers):
            arrived(qrecv.at[p, h], head_recv.at[0, j, h])
            summed = summed + qrecv[p, h].astype(jnp.float32)
        qbuf[h] = (summed * fbuf[...]).astype(jnp.bfloat16)
        for i in range(n_mate):
            mate_send(0, qbuf.at[h], qmate.at[h, pair], h, i)

    def attend(h, query):
        scores = []
        for i in range(4):
            keys = kvbuf[2 * h, 2 * i : 2 * i + 2].reshape(-1, HEAD_DIM)
            scores.append(
                lax.dot_general(
                    query, keys, (((1,), (1,)), ((), ())), preferred_element_type=jnp.float32
                )
            )
        top = scores[0]
        for s in scores[1:]:
            top = jnp.maximum(top, s)
        top = jnp.max(top, axis=1, keepdims=True)
        mixed = jnp.zeros((rows, 2 * HEAD_DIM), jnp.float32)
        for i in range(4):
            vals = kvbuf[2 * h + 1, 2 * i : 2 * i + 2].reshape(-1, HEAD_DIM)
            wide = jnp.concatenate([vals, jnp.ones_like(vals)], axis=1)
            weights = jnp.exp2(scores[i] - top).astype(jnp.bfloat16)
            mixed = mixed + jnp.dot(weights, wide, preferred_element_type=jnp.float32)
        total = mixed[:, HEAD_DIM:]
        return mixed[:, :HEAD_DIM] / total, top + jnp.log(total) * math.log2(math.e)

    def att_own(h):
        opart[h], lse_own[h] = attend(h, qbuf[h])

    def att_mate(h):
        for i, m in enumerate(mates):
            arrived(qmate.at[h, m], mate_recv.at[0, h, i])
            out, lse = attend(h, qmate[h, m])
            osend[h, m] = out.astype(jnp.bfloat16)
            mate_send(1, osend.at[h, m], orecv.at[h, pair], h, i)
            ssend[h, m] = jnp.transpose(lse)[0:8, :]
            mate_send(2, ssend.at[h, m], srecv.at[h, pair], h, i)

    def att_cols(p, h):
        return att.at[:, ds(h * span + p * HEAD_DIM, HEAD_DIM)]

    def merge(h):
        parts = [opart[h]]
        logs = [lse_own[h]]
        for i, m in enumerate(mates):
            arrived(orecv.at[h, m], mate_recv.at[1, h, i])
            arrived(srecv.at[h, m], mate_recv.at[2, h, i])
            parts.append(orecv[h, m].astype(jnp.float32))
            logs.append(jnp.transpose(jnp.broadcast_to(srecv[h, m][0:1, :], (LANES, rows))))
        top = logs[0]
        for log in logs[1:]:
            top = jnp.maximum(top, log)
        shares = [jnp.exp2(log - top) for log in logs]
        total = shares[0]
        mixed = shares[0] * parts[0]
        for share, part in zip(shares[1:], parts[1:]):
            total = total + share
            mixed = mixed + share * part
        att[:, ds(h * span + t * HEAD_DIM, HEAD_DIM)] = (mixed / total).astype(jnp.bfloat16)
        for j, p in enumerate(peers):
            place = head_recv.at[1, n_peer - 1 - j, h]
            remote(att_cols(t, h), att_cols(t, h), 4, place, {"tp": p}).start()

    def att_wait(h):
        for j, p in enumerate(peers):
            arrived(att_cols(p, h), head_recv.at[1, j, h])

    def wo_ref(p, h, q):
        return wo.at[ds(h * span + p * HEAD_DIM + q * wo_rows, wo_rows, wo_rows)]

    def wo_chunk(yy, cc, sub):
        return (yy * 2 + cc) * SUBS + sub

    def wo_start(h, sub):
        q = wo_chunk(side, core, sub)
        for j, p in enumerate(peers):
            src = wo_hbm.at[ds(h * HEAD_DIM + q * wo_rows, wo_rows, wo_rows), ds(p * feat, feat)]
            place = wo_recv.at[n_peer - 1 - j, h, sub]
            remote(src, wo_ref(t, h, q), 8, place, {"tp": p}).start()

    def wo_pass(h, sub):
        for j, p in enumerate(peers):
            ref = wo_ref(p, h, wo_chunk(side, core, sub))
            arrived(ref, wo_recv.at[j, h, sub])
            remote(ref, ref, 8, wo_recv.at[j, h, SUBS + sub], {"blk": beside}).start()
            remote(ref, ref, 8, wo_core_recv.at[j, h], {"blk": sibling}).start()

    def wo_relay(h, sub):
        for j, p in enumerate(peers):
            ref = wo_ref(p, h, wo_chunk(1 - side, core, sub))
            arrived(ref, wo_recv.at[j, h, SUBS + sub])
            remote(ref, ref, 8, wo_core_recv.at[j, h], {"blk": sibling}).start()

    def wo_loaded():
        ref = wo.at[0:width]
        pltpu.make_async_copy(ref, ref, local_sem.at[2]).wait()

    def wo_ready(h):
        for j in range(n_peer):
            arrived(wo.at[0 : HEAD_DIM // 2], wo_core_recv.at[j, h])

    starts = range(0, feat, tile)

    def project_most():
        wo_loaded()
        for h in range(last):
            wo_ready(h)
            att_wait(h)
        for start in starts:
            cols = slice(start, start + tile)
            oacc[:, cols] = jnp.dot(
                att[:, : last * span], wo[: last * span, cols], preferred_element_type=jnp.float32
            )

    events = []

    def at(when, step, *args):
        events.append((when, len(events), step, args))

    for h in range(heads):
        k, v = 2 * h, 2 * h + 1
        stage = max(h - last + 2, 0)
        at(2.0 + 0.1 * h, wq_start, h)
        at(2.45 if h == 0 else 2.6 + 0.01 * h, kv_loaded, h)
        for e in (k, v):
            at(2.5 + 0.01 * e if h == 0 else 12.0 + 0.01 * e, kv_line, e)
            at(2.5 + 0.01 * e if h == 0 else 2.65 if h < last else 9.0, kv_side, e)
            at(2.7 + 0.01 * e, kv_core, e)
        at((6.5, 17.7, 21.9)[stage], kv_from_partner, k)
        at((8.6, 19.8, 24.0)[stage], kv_from_partner, v)
        at((8.7, 12.9, 21.3)[stage], kv_from_beside, k)
        at((8.8, 13.0, 21.4)[stage], kv_from_beside, v)
        at((15.0, 23.3, 26.9)[stage], kv_from_corner, k)
        at((17.0, 24.6, 26.95)[stage], kv_from_corner, v)
        for sub in range(SUBS):
            at((6.4, 9.9, 14.1)[stage] + 1.75 * sub, wq_pass, h, sub)
            at((12.0, 15.6, 17.6)[stage] + (1.75 if h == last else 0.2) * sub, wq_relay, h, sub)
            at(17.5 if stage == 0 and sub == 0 else 21.2 + 0.1 * h, wo_start, h, sub)
            at((26.8, 29.1, 31.6)[stage], wo_pass, h, sub)
            at((31.7, 35.2, 37.1)[stage], wo_relay, h, sub)
        at((13.6, 17.2, 20.7)[stage], q_part, h)
        at((19.8, 22.0, 24.5)[stage], q_make, h)
        at((21.3, 26.98, 29.2)[stage], kv_ready, h)
        at((21.4, 31.8, 33.5)[stage], att_own, h)
        at((24.8, 27.0, 29.5)[stage], att_mate, h)
        at((31.75, 35.0, 37.0)[stage], merge, h)
    at(4.0, norm)
    at(19.7, factor)
    at(37.5, project_most)
    for when, order, step, args in sorted(events, key=lambda event: event[:2]):
        with jax.named_scope("_".join([step.__name__] + [str(a) for a in args])):
            step(*args)

    with jax.named_scope("tail_wait"):
        wo_ready(last)
        att_wait(last)
    for start in starts:
        cols = slice(start, start + tile)
        result = oacc[:, cols] + jnp.dot(
            att[:, last * span :], wo[last * span :, cols], preferred_element_type=jnp.float32
        )
        out_ref[:, cols] = result.astype(jnp.bfloat16)
    with jax.named_scope("drain"):
        sent(kvbuf.at[:, 0:7], 0)
        if n_peer:
            sent(wq.at[0:n_peer], 1)
            sent(sqbuf.at[0:n_peer], 2)
            sent(qsend.at[0:n_peer], 3)
            sent(qsend.at[0:n_peer], 4)
            sent(wo.at[0 : n_peer * width], 8)
        if n_mate:
            sent(qmate.at[:, 0:n_mate], 5)
            sent(osend.at[:, 0:n_mate], 6)
            sent(ssend.at[:, 0:n_mate], 7)


def per_device(n_blk, n_tp, dec_states, norm_gain, query_weight, out_weight, enc_keys, enc_values):
    rows, feat = dec_states.shape
    width = query_weight.shape[1]
    enc_rows = enc_keys.shape[0]
    heads = width // HEAD_DIM
    n_pair = n_blk // 8
    bf16, f32 = jnp.bfloat16, jnp.float32
    dma = pltpu.SemaphoreType.DMA
    anywhere = pl.BlockSpec(memory_space=pl.ANY)
    return pl.pallas_call(
        functools.partial(kernel, n_blk, n_tp),
        out_shape=pltpu.VMEM((rows, feat), bf16),
        in_specs=[
            anywhere,
            anywhere,
            anywhere,
            anywhere,
            anywhere,
            anywhere,
        ],
        out_specs=pl.BlockSpec(memory_space=pltpu.VMEM),
        scratch_shapes=[
            pltpu.VMEM((1, n_tp * feat), f32),
            pltpu.VMEM((2 * heads, 8, enc_rows, HEAD_DIM), bf16),
            pltpu.VMEM((feat, width), bf16),
            pltpu.VMEM((n_tp, heads, feat, HEAD_DIM), bf16),
            pltpu.VMEM((n_tp * width, feat), bf16),
            pltpu.VMEM((rows, feat), bf16),
            pltpu.VMEM((rows, feat), bf16),
            pltpu.VMEM((n_tp, heads, rows, HEAD_DIM), bf16),
            pltpu.VMEM((n_tp, heads, rows, HEAD_DIM), bf16),
            pltpu.VMEM((rows, width), f32),
            pltpu.VMEM((n_tp, 8, rows), f32),
            pltpu.VMEM((rows, LANES), f32),
            pltpu.VMEM((heads, rows, HEAD_DIM), bf16),
            pltpu.VMEM((heads, n_pair, rows, HEAD_DIM), bf16),
            pltpu.VMEM((heads, n_pair, rows, HEAD_DIM), bf16),
            pltpu.VMEM((heads, n_pair, rows, HEAD_DIM), bf16),
            pltpu.VMEM((heads, n_pair, 8, rows), f32),
            pltpu.VMEM((heads, n_pair, 8, rows), f32),
            pltpu.VMEM((heads, rows, HEAD_DIM), f32),
            pltpu.VMEM((heads, rows, LANES), f32),
            pltpu.VMEM((rows, n_tp * width), bf16),
            pltpu.VMEM((rows, feat), f32),
            dma((9,)),
            dma((2 * heads, 3)),
            dma((heads,)),
            dma((n_tp - 1, heads, 2 * SUBS)),
            dma((n_tp - 1, heads)),
            dma((n_tp - 1, heads, 2 * SUBS)),
            dma((n_tp - 1, heads)),
            dma((n_tp - 1,)),
            dma((2, n_tp - 1, heads)),
            dma((3, heads, max(n_pair - 1, 1))),
            dma((heads,)),
            dma((4,)),
        ],
        compiler_params=pltpu.CompilerParams(
            collective_id=0, has_side_effects=True, vmem_limit_bytes=60 * 1024 * 1024
        ),
    )(dec_states, norm_gain.reshape(1, -1), query_weight, out_weight, enc_keys, enc_values)


def solution(mesh):
    in_specs = (P("blk", "tp"), P(), P(None, "tp"), P("tp", None), P("blk", "tp"), P("blk", "tp"))
    out_specs = P("blk", "tp")
    body = functools.partial(per_device, mesh.shape["blk"], mesh.shape["tp"])
    return jax.shard_map(body, mesh=mesh, in_specs=in_specs, out_specs=out_specs, check_vma=False)
```

```python
import functools
import math

import jax
import jax.numpy as jnp
from jax import lax
from jax.experimental import pallas as pl
from jax.experimental.pallas import tpu as pltpu
from jax.sharding import PartitionSpec as P

HEAD_DIM = 128
NORM_EPS = 1e-06
LANES = 128
SUBS = 2


def column_tile(width, limit=640):
    best = LANES
    for tile in range(LANES, limit + 1, LANES):
        if width % tile == 0:
            best = tile
    return best


def kernel(
    n_blk,
    n_tp,
    x_hbm,
    gain_hbm,
    wq_hbm,
    wo_hbm,
    k_hbm,
    v_hbm,
    out_ref,
    gain_ref,
    kvbuf,
    wq_own,
    wq,
    wo,
    xbuf,
    xg,
    qsend,
    qrecv,
    own_part,
    sqbuf,
    fbuf,
    qbuf,
    qmate,
    osend,
    orecv,
    ssend,
    srecv,
    opart,
    lse_own,
    att,
    oacc,
    send_sem,
    kv_recv,
    kv_core_recv,
    wq_recv,
    wq_core_recv,
    wo_recv,
    wo_core_recv,
    sq_recv,
    head_recv,
    mate_recv,
    kv_local,
    local_sem,
):
    n_line = n_blk // 4
    n_pair = n_line // 2
    b = lax.axis_index("blk")
    t = lax.axis_index("tp")
    core = lax.rem(b, 2)
    side = lax.rem(lax.div(b, 2), 2)
    line = lax.div(b, 4)
    par = lax.rem(line, 2)
    pair = lax.div(line, 2)
    rows = x_hbm.shape[0]
    feat = x_hbm.shape[1]
    width = wq_hbm.shape[1]
    heads = width // HEAD_DIM
    span = n_tp * HEAD_DIM
    last = heads - 1
    wq_rows = feat // (4 * SUBS)
    wo_rows = HEAD_DIM // (4 * SUBS)

    def index(zz, yy, cc):
        return (zz * 2 + yy) * 2 + cc

    sibling = index(line, side, 1 - core)
    beside = index(line, 1 - side, core)
    partner = index(line + 1 - 2 * par, side, core)
    peers = [lax.rem(t + off, n_tp) for off in range(1, n_tp)]
    mates = [lax.rem(pair + off, n_pair) for off in range(1, n_pair)]
    n_peer, n_mate = len(peers), len(mates)

    def mate_index(m):
        return index(2 * m + par, side, core)

    def parts_of(h):
        if h < last:
            return [(h, slice(0, rows))]
        return [(h, slice(0, rows // 2)), (h + 1, slice(rows // 2, rows))]

    def ds(start, size, mult=LANES):
        return pl.ds(pl.multiple_of(start, mult), size)

    def head_cols(h):
        return slice(h * HEAD_DIM, (h + 1) * HEAD_DIM)

    def slot(pp, yy, cc):
        return (pp * 2 + yy) * 2 + cc

    mine = slot(par, side, core)

    kv_loads = [
        pltpu.make_async_copy(
            (k_hbm, v_hbm)[e % 2].at[:, head_cols(e // 2)], kvbuf.at[e, mine], kv_local.at[e // 2]
        )
        for e in range(2 * heads)
    ]
    x_load = pltpu.make_async_copy(x_hbm, xbuf, local_sem.at[0])
    gain_load = pltpu.make_async_copy(gain_hbm, gain_ref, local_sem.at[3])
    wq_load = pltpu.make_async_copy(wq_hbm.at[ds(t * feat, feat)], wq_own, local_sem.at[1])
    wo_loads = [
        pltpu.make_async_copy(
            wo_hbm.at[head_cols(h), ds(t * feat, feat)],
            wo.at[ds(h * span + t * HEAD_DIM, HEAD_DIM)],
            local_sem.at[2],
        )
        for h in range(heads)
    ]
    for load in kv_loads[:2] + [gain_load, x_load, wq_load] + kv_loads[2:] + wo_loads:
        load.start()

    barrier = pltpu.get_barrier_semaphore()
    for other in [sibling, beside, partner] + [mate_index(m) for m in mates]:
        pl.semaphore_signal(barrier, inc=1, device_id={"blk": other})
    for p in peers:
        pl.semaphore_signal(barrier, inc=1, device_id={"tp": p})
    pl.semaphore_wait(barrier, 3 + len(mates) + len(peers))

    def remote(src, dst, kind, recv_sem, device_id):
        return pltpu.make_async_remote_copy(
            src_ref=src,
            dst_ref=dst,
            send_sem=send_sem.at[kind],
            recv_sem=recv_sem,
            device_id=device_id,
        )

    def arrived(ref, recv_sem):
        remote(ref, ref, 0, recv_sem, {"blk": sibling}).wait_recv()

    def sent(ref, kind):
        remote(ref, ref, kind, kv_core_recv.at[0], {"blk": sibling}).wait_send()

    def kv_send(e, s, kind, target):
        ref = kvbuf.at[e, s]
        remote(ref, ref, 0, kv_recv.at[e, kind], {"blk": target}).start()

    def kv_share(e, s):
        ref = kvbuf.at[e, s]
        remote(ref, ref, 0, kv_core_recv.at[e // 2], {"blk": sibling}).start()

    def kv_wait(e, s, kind):
        arrived(kvbuf.at[e, s], kv_recv.at[e, kind])

    from_beside = slot(par, 1 - side, core)
    from_partner = slot(1 - par, side, core)
    from_corner = slot(1 - par, 1 - side, core)

    by_line = (2 * heads - 1,)

    def kv_loaded(h):
        both = kvbuf.at[2 * h : 2 * h + 2, mine]
        pltpu.make_async_copy(both, both, kv_local.at[h]).wait()

    def kv_line(e):
        kv_send(e, mine, 1, partner)

    def kv_side(e):
        kv_send(e, mine, 0, beside)

    def kv_core(e):
        kv_share(e, mine)

    def kv_from_partner(e):
        kv_wait(e, from_partner, 1)
        if e not in by_line:
            kv_send(e, from_partner, 2, beside)
        kv_share(e, from_partner)

    def kv_from_beside(e):
        kv_wait(e, from_beside, 0)
        if e in by_line:
            kv_send(e, from_beside, 2, partner)
        kv_share(e, from_beside)

    def kv_from_corner(e):
        kv_wait(e, from_corner, 2)
        kv_share(e, from_corner)

    def kv_ready(h):
        arrived(kvbuf.at[2 * h : 2 * h + 2, 0:4], kv_core_recv.at[h])

    def wq_chunk(pp, cc, sub):
        return (pp * 2 + cc) * SUBS + sub

    def wq_ref(p, h, c):
        return wq.at[p, h, ds(c * wq_rows, wq_rows, 16)]

    def wq_hop(j, h, c, k):
        ref = wq_ref(peers[j], h, c)
        remote(ref, ref, 1, wq_recv.at[j, h, k], {"blk": partner}).start()

    def wq_share(j, h, c):
        ref = wq_ref(peers[j], h, c)
        remote(ref, ref, 1, wq_core_recv.at[j, h], {"blk": sibling}).start()

    def wq_start(h):
        for k in range(2 * SUBS if h == last else SUBS):
            for j, p in enumerate(peers):
                c = wq_chunk(par if k < SUBS else 1 - par, core, k % SUBS)
                src = wq_hbm.at[ds(p * feat + c * wq_rows, wq_rows, 16), head_cols(h)]
                place = wq_recv.at[n_peer - 1 - j, h, k]
                remote(src, wq_ref(t, h, c), 1, place, {"tp": p}).start()

    def wq_pass(h, sub):
        for j, p in enumerate(peers):
            c = wq_chunk(par, core, sub)
            arrived(wq_ref(p, h, c), wq_recv.at[j, h, sub])
            if h != last:
                wq_hop(j, h, c, SUBS + sub)
            wq_share(j, h, c)

    def wq_relay(h, sub):
        for j, p in enumerate(peers):
            c = wq_chunk(1 - par, core, sub)
            arrived(wq_ref(p, h, c), wq_recv.at[j, h, SUBS + sub])
            wq_share(j, h, c)

    def q_part(h):
        for j, p in enumerate(peers):
            arrived(wq.at[p, h, 0 : feat // 2], wq_core_recv.at[j, h])
            qsend[p, h] = jnp.dot(
                xg[...], wq[p, h], preferred_element_type=jnp.float32
            ).astype(jnp.bfloat16)
            for place, part in parts_of(h):
                remote(
                    qsend.at[p, h, part],
                    qrecv.at[t, h, part],
                    3,
                    head_recv.at[0, n_peer - 1 - j, place],
                    {"tp": p},
                ).start()

    tile = column_tile(feat)

    def norm():
        gain_load.wait()
        x_load.wait()
        squares = jnp.zeros((rows, 1), jnp.float32)
        for start in range(0, feat, tile):
            piece = xbuf[:, start : start + tile].astype(jnp.float32)
            squares += jnp.sum(piece * piece, axis=1, keepdims=True)
            gain = gain_ref[:, ds(t * feat + start, tile)]
            xg[:, start : start + tile] = (piece * gain).astype(jnp.bfloat16)
        wide = jnp.broadcast_to(squares, (rows, LANES))
        sqbuf[t] = jnp.transpose(wide)[0:8, :]
        for j, p in enumerate(peers):
            ref = sqbuf.at[t]
            remote(ref, ref, 2, sq_recv.at[n_peer - 1 - j], {"tp": p}).start()
        wq_load.wait()
        own_part[...] = jnp.dot(xg[...], wq_own[...], preferred_element_type=jnp.float32)

    def factor():
        total = sqbuf[t][0:1, :]
        for j, p in enumerate(peers):
            arrived(sqbuf.at[p], sq_recv.at[j])
            total = total + sqbuf[p][0:1, :]
        column = jnp.transpose(jnp.broadcast_to(total, (LANES, rows)))
        scale = math.log2(math.e) / math.sqrt(HEAD_DIM)
        fbuf[...] = lax.rsqrt(column / (feat * n_tp) + NORM_EPS) * scale

    def mate_send(k, src, dst, place, i):
        there = mate_recv.at[k, place, n_mate - 1 - i]
        remote(src, dst, 5 + k, there, {"blk": mate_index(mates[i])}).start()

    def q_make(h, b):
        place, part = parts_of(h)[b]
        summed = own_part[part, head_cols(h)]
        for j, p in enumerate(peers):
            arrived(qrecv.at[p, h, part], head_recv.at[0, j, place])
            summed = summed + qrecv[p, h, part].astype(jnp.float32)
        qbuf[h, part] = (summed * fbuf[part]).astype(jnp.bfloat16)
        for i in range(n_mate):
            mate_send(0, qbuf.at[h, part], qmate.at[h, pair, part], place, i)

    def attend(h, query, emit):
        half = rows // 2

        def score(b):
            block = query(b, slice(b * half, b * half + half))
            scores = []
            for i in range(4):
                keys = kvbuf[2 * h, 2 * i : 2 * i + 2].reshape(-1, HEAD_DIM)
                scores.append(
                    lax.dot_general(
                        block, keys, (((1,), (1,)), ((), ())), preferred_element_type=jnp.float32
                    )
                )
            return scores

        later = score(0)
        for b in range(2):
            scores = later
            if b == 0:
                later = score(1)
            top = scores[0]
            for s in scores[1:]:
                top = jnp.maximum(top, s)
            top = jnp.max(top, axis=1, keepdims=True)
            mixed = jnp.zeros((half, 2 * HEAD_DIM), jnp.float32)
            for i in range(4):
                vals = kvbuf[2 * h + 1, 2 * i : 2 * i + 2].reshape(-1, HEAD_DIM)
                wide = jnp.concatenate([vals, jnp.ones_like(vals)], axis=1)
                weights = jnp.exp2(scores[i] - top).astype(jnp.bfloat16)
                mixed = mixed + jnp.dot(weights, wide, preferred_element_type=jnp.float32)
            total = mixed[:, HEAD_DIM:]
            lse = top + jnp.log(total) * math.log2(math.e)
            emit(b, slice(b * half, b * half + half), mixed[:, :HEAD_DIM] / total, lse)

    def att_own(h):
        def emit(b, part, out, lse):
            opart[h, part] = out
            lse_own[h, part] = lse

        attend(h, lambda b, part: qbuf[h, part], emit)

    def att_mate(h):
        for i, m in enumerate(mates):

            def query(b, part):
                if b < len(parts_of(h)):
                    place, piece = parts_of(h)[b]
                    arrived(qmate.at[h, m, piece], mate_recv.at[0, place, i])
                return qmate[h, m, part]

            def emit(b, part, out, lse):
                osend[h, m, part] = out.astype(jnp.bfloat16)
                ssend[h, m, :, part] = jnp.transpose(lse)[0:8, :]
                if b == 1 or len(parts_of(h)) == 2:
                    place, piece = parts_of(h)[min(b, len(parts_of(h)) - 1)]
                    mate_send(1, osend.at[h, m, piece], orecv.at[h, pair, piece], place, i)
                    here, there = ssend.at[h, m, :, piece], srecv.at[h, pair, :, piece]
                    mate_send(2, here, there, place, i)

            attend(h, query, emit)

    def att_ref(p, h, part):
        return att.at[part, ds(h * span + p * HEAD_DIM, HEAD_DIM)]

    def merge(h, b):
        place, part = parts_of(h)[b]
        parts = [opart[h, part]]
        logs = [lse_own[h, part]]
        for i, m in enumerate(mates):
            arrived(srecv.at[h, m, :, part], mate_recv.at[2, place, i])
            arrived(orecv.at[h, m, part], mate_recv.at[1, place, i])
            parts.append(orecv[h, m, part].astype(jnp.float32))
            stat = srecv[h, m, 0:1, part]
            logs.append(jnp.transpose(jnp.broadcast_to(stat, (LANES, stat.shape[1]))))
        top = logs[0]
        for log in logs[1:]:
            top = jnp.maximum(top, log)
        shares = [jnp.exp2(log - top) for log in logs]
        total = shares[0]
        mixed = shares[0] * parts[0]
        for share, piece in zip(shares[1:], parts[1:]):
            total = total + share
            mixed = mixed + share * piece
        att[part, ds(h * span + t * HEAD_DIM, HEAD_DIM)] = (mixed / total).astype(jnp.bfloat16)
        for j, p in enumerate(peers):
            there = head_recv.at[1, n_peer - 1 - j, place]
            remote(att_ref(t, h, part), att_ref(t, h, part), 4, there, {"tp": p}).start()

    def att_wait(h, b):
        place, part = parts_of(h)[b]
        for j, p in enumerate(peers):
            arrived(att_ref(p, h, part), head_recv.at[1, j, place])

    def wo_ref(p, h, q):
        return wo.at[ds(h * span + p * HEAD_DIM + q * wo_rows, wo_rows, wo_rows)]

    def wo_chunk(yy, cc, sub):
        return (yy * 2 + cc) * SUBS + sub

    def wo_start(h, sub):
        q = wo_chunk(side, core, sub)
        for j, p in enumerate(peers):
            src = wo_hbm.at[ds(h * HEAD_DIM + q * wo_rows, wo_rows, wo_rows), ds(p * feat, feat)]
            place = wo_recv.at[n_peer - 1 - j, h, sub]
            remote(src, wo_ref(t, h, q), 8, place, {"tp": p}).start()

    def wo_pass(h, sub):
        for j, p in enumerate(peers):
            ref = wo_ref(p, h, wo_chunk(side, core, sub))
            arrived(ref, wo_recv.at[j, h, sub])
            remote(ref, ref, 8, wo_recv.at[j, h, SUBS + sub], {"blk": beside}).start()
            remote(ref, ref, 8, wo_core_recv.at[j, h], {"blk": sibling}).start()

    def wo_relay(h, sub):
        for j, p in enumerate(peers):
            ref = wo_ref(p, h, wo_chunk(1 - side, core, sub))
            arrived(ref, wo_recv.at[j, h, SUBS + sub])
            remote(ref, ref, 8, wo_core_recv.at[j, h], {"blk": sibling}).start()

    def wo_loaded():
        ref = wo.at[0:width]
        pltpu.make_async_copy(ref, ref, local_sem.at[2]).wait()

    def wo_ready(h):
        for j in range(n_peer):
            arrived(wo.at[0 : HEAD_DIM // 2], wo_core_recv.at[j, h])

    starts = range(0, feat, tile)

    def project_most():
        wo_loaded()
        for h in range(last):
            wo_ready(h)
            att_wait(h, 0)
        for start in starts:
            cols = slice(start, start + tile)
            oacc[:, cols] = jnp.dot(
                att[:, : last * span], wo[: last * span, cols], preferred_element_type=jnp.float32
            )

    events = []

    def at(when, step, *args):
        events.append((when, len(events), step, args))

    for h in range(heads):
        k, v = 2 * h, 2 * h + 1
        stage = max(h - last + 2, 0)
        at(2.0 + 0.1 * h, wq_start, h)
        at(2.45 if h == 0 else 2.6 + 0.01 * h, kv_loaded, h)
        for e in (k, v):
            at(2.5 + 0.01 * e if h == 0 else 9.36 + 0.001 * e, kv_line, e)
            at(2.5 + 0.01 * e if h == 0 else 2.65 if h < last else 7.05, kv_side, e)
            at(2.7 + 0.01 * e, kv_core, e)
        at((4.9, 16.3, 20.5)[stage], kv_from_partner, k)
        at((7.0, 18.1, 23.4)[stage], kv_from_partner, v)
        at((7.1, 9.4, 20.6)[stage], kv_from_beside, k)
        at((7.2, 10.8, 20.7)[stage], kv_from_beside, v)
        at((12.6, 21.7, 26.7)[stage], kv_from_corner, k)
        at((14.6, 24.0, 26.8)[stage], kv_from_corner, v)
        for sub in range(SUBS):
            at((4.2, 7.6, 11.2)[stage] + 1.75 * sub, wq_pass, h, sub)
            at((10.2, 14.2, 14.7)[stage] + (1.75 if h == last else 0.1) * sub, wq_relay, h, sub)
            at(15.6 if stage == 0 and sub == 0 else 18.0 + 0.1 * h, wo_start, h, sub)
            at((23.5, 27.7, 30.3)[stage], wo_pass, h, sub)
            at((30.4, 32.0, 34.1)[stage], wo_relay, h, sub)
        at((12.0, 15.5, 17.7)[stage], q_part, h)
        at((17.9, 19.6, 20.9)[stage], q_make, h, 0)
        at((18.1, 25.3, 27.75)[stage], kv_ready, h)
        at((18.2, 26.9, 29.6)[stage], att_own, h)
        at((22.0, 25.4, 27.8)[stage], att_mate, h)
        at((30.35, 31.9, 33.2)[stage], merge, h, 0)
    at(21.4, q_make, last, 1)
    at(34.0, merge, last, 1)
    at(4.0, norm)
    at(17.85, factor)
    at(37.5, project_most)
    for when, order, step, args in sorted(events, key=lambda event: event[:2]):
        with jax.named_scope("_".join([step.__name__] + [str(a) for a in args])):
            step(*args)

    wo_ready(last)
    for b, (place, part) in enumerate(parts_of(last)):
        with jax.named_scope(f"tail_wait_{b}"):
            att_wait(last, b)
        for start in starts:
            cols = slice(start, start + tile)
            result = oacc[part, cols] + jnp.dot(
                att[part, last * span :],
                wo[last * span :, cols],
                preferred_element_type=jnp.float32,
            )
            out_ref[part, cols] = result.astype(jnp.bfloat16)
    with jax.named_scope("drain"):
        sent(kvbuf.at[:, 0:7], 0)
        if n_peer:
            sent(wq.at[0:n_peer], 1)
            sent(sqbuf.at[0:n_peer], 2)
            sent(qsend.at[0:n_peer], 3)
            sent(qsend.at[0:n_peer], 4)
            sent(wo.at[0 : n_peer * width], 8)
        if n_mate:
            sent(qmate.at[:, 0:n_mate], 5)
            sent(osend.at[:, 0:n_mate], 6)
            sent(ssend.at[:, 0:n_mate], 7)


def per_device(n_blk, n_tp, dec_states, norm_gain, query_weight, out_weight, enc_keys, enc_values):
    rows, feat = dec_states.shape
    width = query_weight.shape[1]
    enc_rows = enc_keys.shape[0]
    heads = width // HEAD_DIM
    n_pair = n_blk // 8
    bf16, f32 = jnp.bfloat16, jnp.float32
    dma = pltpu.SemaphoreType.DMA
    anywhere = pl.BlockSpec(memory_space=pl.ANY)
    return pl.pallas_call(
        functools.partial(kernel, n_blk, n_tp),
        out_shape=pltpu.VMEM((rows, feat), bf16),
        in_specs=[
            anywhere,
            anywhere,
            anywhere,
            anywhere,
            anywhere,
            anywhere,
        ],
        out_specs=pl.BlockSpec(memory_space=pltpu.VMEM),
        scratch_shapes=[
            pltpu.VMEM((1, n_tp * feat), f32),
            pltpu.VMEM((2 * heads, 8, enc_rows, HEAD_DIM), bf16),
            pltpu.VMEM((feat, width), bf16),
            pltpu.VMEM((n_tp, heads, feat, HEAD_DIM), bf16),
            pltpu.VMEM((n_tp * width, feat), bf16),
            pltpu.VMEM((rows, feat), bf16),
            pltpu.VMEM((rows, feat), bf16),
            pltpu.VMEM((n_tp, heads, rows, HEAD_DIM), bf16),
            pltpu.VMEM((n_tp, heads, rows, HEAD_DIM), bf16),
            pltpu.VMEM((rows, width), f32),
            pltpu.VMEM((n_tp, 8, rows), f32),
            pltpu.VMEM((rows, LANES), f32),
            pltpu.VMEM((heads, rows, HEAD_DIM), bf16),
            pltpu.VMEM((heads, n_pair, rows, HEAD_DIM), bf16),
            pltpu.VMEM((heads, n_pair, rows, HEAD_DIM), bf16),
            pltpu.VMEM((heads, n_pair, rows, HEAD_DIM), bf16),
            pltpu.VMEM((heads, n_pair, 8, rows), f32),
            pltpu.VMEM((heads, n_pair, 8, rows), f32),
            pltpu.VMEM((heads, rows, HEAD_DIM), f32),
            pltpu.VMEM((heads, rows, LANES), f32),
            pltpu.VMEM((rows, n_tp * width), bf16),
            pltpu.VMEM((rows, feat), f32),
            dma((9,)),
            dma((2 * heads, 3)),
            dma((heads,)),
            dma((n_tp - 1, heads, 2 * SUBS)),
            dma((n_tp - 1, heads)),
            dma((n_tp - 1, heads, 2 * SUBS)),
            dma((n_tp - 1, heads)),
            dma((n_tp - 1,)),
            dma((2, n_tp - 1, heads + 1)),
            dma((3, heads + 1, max(n_pair - 1, 1))),
            dma((heads,)),
            dma((4,)),
        ],
        compiler_params=pltpu.CompilerParams(
            collective_id=0, has_side_effects=True, vmem_limit_bytes=60 * 1024 * 1024
        ),
    )(dec_states, norm_gain.reshape(1, -1), query_weight, out_weight, enc_keys, enc_values)


def solution(mesh):
    in_specs = (P("blk", "tp"), P(), P(None, "tp"), P("tp", None), P("blk", "tp"), P("blk", "tp"))
    out_specs = P("blk", "tp")
    body = functools.partial(per_device, mesh.shape["blk"], mesh.shape["tp"])
    return jax.shard_map(body, mesh=mesh, in_specs=in_specs, out_specs=out_specs, check_vma=False)
```

```python
import functools
import math

import jax
import jax.numpy as jnp
from jax import lax
from jax.experimental import pallas as pl
from jax.experimental.pallas import tpu as pltpu
from jax.sharding import PartitionSpec as P

HEAD_DIM = 128
NORM_EPS = 1e-06
LANES = 128
SUBS = 2


def column_tile(width, limit=640):
    best = LANES
    for tile in range(LANES, limit + 1, LANES):
        if width % tile == 0:
            best = tile
    return best


def kernel(
    n_blk,
    n_tp,
    x_hbm,
    gain_hbm,
    wq_hbm,
    wo_hbm,
    k_hbm,
    v_hbm,
    out_ref,
    gain_ref,
    kvbuf,
    wq_own,
    wq,
    wo,
    xbuf,
    xg,
    qsend,
    qrecv,
    own_part,
    sqbuf,
    fbuf,
    qbuf,
    qmate,
    osend,
    orecv,
    ssend,
    srecv,
    opart,
    lse_own,
    att,
    oacc,
    send_sem,
    kv_recv,
    kv_core_recv,
    wq_recv,
    wq_core_recv,
    wo_recv,
    wo_core_recv,
    sq_recv,
    head_recv,
    mate_recv,
    kv_local,
    local_sem,
):
    n_line = n_blk // 4
    n_pair = n_line // 2
    b = lax.axis_index("blk")
    t = lax.axis_index("tp")
    core = lax.rem(b, 2)
    side = lax.rem(lax.div(b, 2), 2)
    line = lax.div(b, 4)
    par = lax.rem(line, 2)
    pair = lax.div(line, 2)
    rows = x_hbm.shape[0]
    feat = x_hbm.shape[1]
    width = wq_hbm.shape[1]
    heads = width // HEAD_DIM
    span = n_tp * HEAD_DIM
    last = heads - 1
    wq_rows = feat // (4 * SUBS)
    wo_rows = HEAD_DIM // (4 * SUBS)

    def index(zz, yy, cc):
        return (zz * 2 + yy) * 2 + cc

    sibling = index(line, side, 1 - core)
    beside = index(line, 1 - side, core)
    partner = index(line + 1 - 2 * par, side, core)
    peers = [lax.rem(t + off, n_tp) for off in range(1, n_tp)]
    mates = [lax.rem(pair + off, n_pair) for off in range(1, n_pair)]
    n_peer, n_mate = len(peers), len(mates)

    def mate_index(m):
        return index(2 * m + par, side, core)

    def parts_of(h):
        if h < last:
            return [(h, slice(0, rows))]
        return [(h, slice(0, rows // 2)), (h + 1, slice(rows // 2, rows))]

    def ds(start, size, mult=LANES):
        return pl.ds(pl.multiple_of(start, mult), size)

    def head_cols(h):
        return slice(h * HEAD_DIM, (h + 1) * HEAD_DIM)

    def slot(pp, yy, cc):
        return (pp * 2 + yy) * 2 + cc

    mine = slot(par, side, core)

    kv_loads = [
        pltpu.make_async_copy(
            (k_hbm, v_hbm)[e % 2].at[:, head_cols(e // 2)], kvbuf.at[e, mine], kv_local.at[e // 2]
        )
        for e in range(2 * heads)
    ]
    x_load = pltpu.make_async_copy(x_hbm, xbuf, local_sem.at[0])
    gain_load = pltpu.make_async_copy(gain_hbm, gain_ref, local_sem.at[3])
    wq_load = pltpu.make_async_copy(wq_hbm.at[ds(t * feat, feat)], wq_own, local_sem.at[1])
    wo_loads = [
        pltpu.make_async_copy(
            wo_hbm.at[head_cols(h), ds(t * feat, feat)],
            wo.at[ds(h * span + t * HEAD_DIM, HEAD_DIM)],
            local_sem.at[2],
        )
        for h in range(heads)
    ]
    for load in kv_loads[:2] + [gain_load, x_load, wq_load] + kv_loads[2:] + wo_loads:
        load.start()

    barrier = pltpu.get_barrier_semaphore()
    for other in [sibling, beside, partner] + [mate_index(m) for m in mates]:
        pl.semaphore_signal(barrier, inc=1, device_id={"blk": other})
    for p in peers:
        pl.semaphore_signal(barrier, inc=1, device_id={"tp": p})
    pl.semaphore_wait(barrier, 3 + len(mates) + len(peers))

    def remote(src, dst, kind, recv_sem, device_id):
        return pltpu.make_async_remote_copy(
            src_ref=src,
            dst_ref=dst,
            send_sem=send_sem.at[kind],
            recv_sem=recv_sem,
            device_id=device_id,
        )

    def arrived(ref, recv_sem):
        remote(ref, ref, 0, recv_sem, {"blk": sibling}).wait_recv()

    def sent(ref, kind):
        remote(ref, ref, kind, kv_core_recv.at[0], {"blk": sibling}).wait_send()

    def kv_send(e, s, kind, target):
        ref = kvbuf.at[e, s]
        remote(ref, ref, 0, kv_recv.at[e, kind], {"blk": target}).start()

    def kv_share(e, s):
        ref = kvbuf.at[e, s]
        remote(ref, ref, 0, kv_core_recv.at[e // 2], {"blk": sibling}).start()

    def kv_wait(e, s, kind):
        arrived(kvbuf.at[e, s], kv_recv.at[e, kind])

    from_beside = slot(par, 1 - side, core)
    from_partner = slot(1 - par, side, core)
    from_corner = slot(1 - par, 1 - side, core)

    by_line = ()

    def kv_loaded(h):
        both = kvbuf.at[2 * h : 2 * h + 2, mine]
        pltpu.make_async_copy(both, both, kv_local.at[h]).wait()

    def kv_line(e):
        kv_send(e, mine, 1, partner)

    def kv_side(e):
        kv_send(e, mine, 0, beside)

    def kv_core(e):
        kv_share(e, mine)

    def kv_from_partner(e):
        kv_wait(e, from_partner, 1)
        if e not in by_line:
            kv_send(e, from_partner, 2, beside)
        kv_share(e, from_partner)

    def kv_from_beside(e):
        kv_wait(e, from_beside, 0)
        if e in by_line:
            kv_send(e, from_beside, 2, partner)
        kv_share(e, from_beside)

    def kv_from_corner(e):
        kv_wait(e, from_corner, 2)
        kv_share(e, from_corner)

    def kv_ready(h):
        arrived(kvbuf.at[2 * h : 2 * h + 2, 0:4], kv_core_recv.at[h])

    def wq_chunk(pp, cc, sub):
        return (pp * 2 + cc) * SUBS + sub

    def wq_ref(p, h, c):
        return wq.at[p, h, ds(c * wq_rows, wq_rows, 16)]

    def wq_hop(j, h, c, k):
        ref = wq_ref(peers[j], h, c)
        remote(ref, ref, 1, wq_recv.at[j, h, k], {"blk": partner}).start()

    def wq_share(j, h, c):
        ref = wq_ref(peers[j], h, c)
        remote(ref, ref, 1, wq_core_recv.at[j, h], {"blk": sibling}).start()

    def wq_start(h, k):
        for j, p in enumerate(peers):
            c = wq_chunk(par if k < SUBS else 1 - par, core, k % SUBS)
            src = wq_hbm.at[ds(p * feat + c * wq_rows, wq_rows, 16), head_cols(h)]
            place = wq_recv.at[n_peer - 1 - j, h, k]
            remote(src, wq_ref(t, h, c), 1, place, {"tp": p}).start()

    def wq_pass(h, sub):
        for j, p in enumerate(peers):
            c = wq_chunk(par, core, sub)
            arrived(wq_ref(p, h, c), wq_recv.at[j, h, sub])
            if h != last:
                wq_hop(j, h, c, SUBS + sub)
            wq_share(j, h, c)

    def wq_relay(h, sub):
        for j, p in enumerate(peers):
            c = wq_chunk(1 - par, core, sub)
            arrived(wq_ref(p, h, c), wq_recv.at[j, h, SUBS + sub])
            wq_share(j, h, c)

    def q_part(h):
        for j, p in enumerate(peers):
            arrived(wq.at[p, h, 0 : feat // 2], wq_core_recv.at[j, h])
            qsend[p, h] = jnp.dot(
                xg[...], wq[p, h], preferred_element_type=jnp.float32
            ).astype(jnp.bfloat16)
            for place, part in parts_of(h):
                remote(
                    qsend.at[p, h, part],
                    qrecv.at[t, h, part],
                    3,
                    head_recv.at[0, n_peer - 1 - j, place],
                    {"tp": p},
                ).start()

    tile = column_tile(feat)

    def norm():
        gain_load.wait()
        x_load.wait()
        squares = jnp.zeros((rows, 1), jnp.float32)
        for start in range(0, feat, tile):
            piece = xbuf[:, start : start + tile].astype(jnp.float32)
            squares += jnp.sum(piece * piece, axis=1, keepdims=True)
            gain = gain_ref[:, ds(t * feat + start, tile)]
            xg[:, start : start + tile] = (piece * gain).astype(jnp.bfloat16)
        wide = jnp.broadcast_to(squares, (rows, LANES))
        sqbuf[t] = jnp.transpose(wide)[0:8, :]
        for j, p in enumerate(peers):
            ref = sqbuf.at[t]
            remote(ref, ref, 2, sq_recv.at[n_peer - 1 - j], {"tp": p}).start()
        wq_load.wait()
        own_part[...] = jnp.dot(xg[...], wq_own[...], preferred_element_type=jnp.float32)

    def factor():
        total = sqbuf[t][0:1, :]
        for j, p in enumerate(peers):
            arrived(sqbuf.at[p], sq_recv.at[j])
            total = total + sqbuf[p][0:1, :]
        column = jnp.transpose(jnp.broadcast_to(total, (LANES, rows)))
        scale = math.log2(math.e) / math.sqrt(HEAD_DIM)
        fbuf[...] = lax.rsqrt(column / (feat * n_tp) + NORM_EPS) * scale

    def mate_send(k, src, dst, place, i):
        there = mate_recv.at[k, place, n_mate - 1 - i]
        remote(src, dst, 5 + k, there, {"blk": mate_index(mates[i])}).start()

    def q_make(h, b):
        place, part = parts_of(h)[b]
        summed = own_part[part, head_cols(h)]
        for j, p in enumerate(peers):
            arrived(qrecv.at[p, h, part], head_recv.at[0, j, place])
            summed = summed + qrecv[p, h, part].astype(jnp.float32)
        qbuf[h, part] = (summed * fbuf[part]).astype(jnp.bfloat16)
        for i in range(n_mate):
            mate_send(0, qbuf.at[h, part], qmate.at[h, pair, part], place, i)

    def attend(h, query, emit):
        half = rows // 2

        def score(b):
            block = query(b, slice(b * half, b * half + half))
            scores = []
            for i in range(4):
                keys = kvbuf[2 * h, 2 * i : 2 * i + 2].reshape(-1, HEAD_DIM)
                scores.append(
                    lax.dot_general(
                        block, keys, (((1,), (1,)), ((), ())), preferred_element_type=jnp.float32
                    )
                )
            return scores

        later = score(0)
        for b in range(2):
            scores = later
            if b == 0:
                later = score(1)
            top = scores[0]
            for s in scores[1:]:
                top = jnp.maximum(top, s)
            top = jnp.max(top, axis=1, keepdims=True)
            mixed = jnp.zeros((half, 2 * HEAD_DIM), jnp.float32)
            for i in range(4):
                vals = kvbuf[2 * h + 1, 2 * i : 2 * i + 2].reshape(-1, HEAD_DIM)
                wide = jnp.concatenate([vals, jnp.ones_like(vals)], axis=1)
                weights = jnp.exp2(scores[i] - top).astype(jnp.bfloat16)
                mixed = mixed + jnp.dot(weights, wide, preferred_element_type=jnp.float32)
            total = mixed[:, HEAD_DIM:]
            lse = top + jnp.log(total) * math.log2(math.e)
            emit(b, slice(b * half, b * half + half), mixed[:, :HEAD_DIM] / total, lse)

    def att_own(h):
        def emit(b, part, out, lse):
            opart[h, part] = out
            lse_own[h, part] = lse

        attend(h, lambda b, part: qbuf[h, part], emit)

    def o_send(h, b):
        place, part = parts_of(h)[b]
        for i, m in enumerate(mates):
            mate_send(1, osend.at[h, m, part], orecv.at[h, pair, part], place, i)
            here, there = ssend.at[h, m, :, part], srecv.at[h, pair, :, part]
            mate_send(2, here, there, place, i)

    def att_mate(h):
        for i, m in enumerate(mates):

            def query(b, part):
                if b < len(parts_of(h)):
                    place, piece = parts_of(h)[b]
                    arrived(qmate.at[h, m, piece], mate_recv.at[0, place, i])
                return qmate[h, m, part]

            def emit(b, part, out, lse):
                osend[h, m, part] = out.astype(jnp.bfloat16)
                ssend[h, m, :, part] = jnp.transpose(lse)[0:1, :]
                if h == last:
                    o_send(h, b)

            attend(h, query, emit)

    def att_ref(p, h, part):
        return att.at[part, ds(h * span + p * HEAD_DIM, HEAD_DIM)]

    def merge(h, b):
        place, part = parts_of(h)[b]
        parts = [opart[h, part]]
        logs = [lse_own[h, part]]
        for i, m in enumerate(mates):
            arrived(srecv.at[h, m, :, part], mate_recv.at[2, place, i])
            arrived(orecv.at[h, m, part], mate_recv.at[1, place, i])
            parts.append(orecv[h, m, part].astype(jnp.float32))
            stat = srecv[h, m, :, part]
            logs.append(jnp.transpose(jnp.broadcast_to(stat, (LANES, stat.shape[1]))))
        top = logs[0]
        for log in logs[1:]:
            top = jnp.maximum(top, log)
        shares = [jnp.exp2(log - top) for log in logs]
        total = shares[0]
        mixed = shares[0] * parts[0]
        for share, piece in zip(shares[1:], parts[1:]):
            total = total + share
            mixed = mixed + share * piece
        att[part, ds(h * span + t * HEAD_DIM, HEAD_DIM)] = (mixed / total).astype(jnp.bfloat16)
        for j, p in enumerate(peers):
            there = head_recv.at[1, n_peer - 1 - j, place]
            remote(att_ref(t, h, part), att_ref(t, h, part), 4, there, {"tp": p}).start()

    def att_wait(h, b):
        place, part = parts_of(h)[b]
        for j, p in enumerate(peers):
            arrived(att_ref(p, h, part), head_recv.at[1, j, place])

    def wo_ref(p, h, q):
        return wo.at[ds(h * span + p * HEAD_DIM + q * wo_rows, wo_rows, wo_rows)]

    def wo_chunk(yy, cc, sub):
        return (yy * 2 + cc) * SUBS + sub

    def wo_half(h):
        return par if h == last else side

    def wo_start(h, sub):
        q = wo_chunk(wo_half(h), core, sub)
        for j, p in enumerate(peers):
            src = wo_hbm.at[ds(h * HEAD_DIM + q * wo_rows, wo_rows, wo_rows), ds(p * feat, feat)]
            place = wo_recv.at[n_peer - 1 - j, h, sub]
            remote(src, wo_ref(t, h, q), 8, place, {"tp": p}).start()

    def wo_pass(h, sub):
        target = partner if h == last else beside
        for j, p in enumerate(peers):
            ref = wo_ref(p, h, wo_chunk(wo_half(h), core, sub))
            arrived(ref, wo_recv.at[j, h, sub])
            remote(ref, ref, 8, wo_recv.at[j, h, SUBS + sub], {"blk": target}).start()
            remote(ref, ref, 8, wo_core_recv.at[j, h], {"blk": sibling}).start()

    def wo_relay(h, sub):
        for j, p in enumerate(peers):
            ref = wo_ref(p, h, wo_chunk(1 - wo_half(h), core, sub))
            arrived(ref, wo_recv.at[j, h, SUBS + sub])
            remote(ref, ref, 8, wo_core_recv.at[j, h], {"blk": sibling}).start()

    def wo_loaded():
        ref = wo.at[0:width]
        pltpu.make_async_copy(ref, ref, local_sem.at[2]).wait()

    def wo_ready(h):
        for j in range(n_peer):
            arrived(wo.at[0 : HEAD_DIM // 2], wo_core_recv.at[j, h])

    starts = range(0, feat, tile)

    def project(h):
        if h == 0:
            wo_loaded()
        wo_ready(h)
        att_wait(h, 0)
        for start in starts:
            cols = slice(start, start + tile)
            block = slice(h * span, (h + 1) * span)
            result = jnp.dot(att[:, block], wo[block, cols], preferred_element_type=jnp.float32)
            oacc[:, cols] = result if h == 0 else oacc[:, cols] + result

    events = []

    def at(when, step, *args):
        events.append((when, len(events), step, args))

    for h in range(heads):
        k, v = 2 * h, 2 * h + 1
        stage = max(h - last + 2, 0)
        for piece in range(2 * SUBS if h == last else SUBS):
            at(12.01 if piece >= 2 * SUBS - 1 else 2.0 + 0.1 * h, wq_start, h, piece)
        at(2.45 if h == 0 else 2.6 + 0.01 * h, kv_loaded, h)
        for e in (k, v):
            at((2.5 + 0.01 * e, 9.36, 14.25 if e == k else 16.55)[stage], kv_line, e)
            at((2.5 + 0.01 * e, 2.65, 7.05)[stage], kv_side, e)
            at(2.7 + 0.01 * e, kv_core, e)
        at((4.9, 16.2, 21.85)[stage], kv_from_partner, k)
        at((7.0, 18.1, 24.6)[stage], kv_from_partner, v)
        at((7.1, 9.4, 20.2)[stage], kv_from_beside, k)
        at((7.2, 10.8, 20.3)[stage], kv_from_beside, v)
        at((12.6, 22.6, 27.1)[stage], kv_from_corner, k)
        at((14.6, 24.7, 28.2)[stage], kv_from_corner, v)
        for sub in range(SUBS):
            at((4.2, 7.6, 11.2)[stage] + 1.75 * sub, wq_pass, h, sub)
            at((10.2, 14.2, 15.2)[stage] + (3.3 if h == last else 0.1) * sub, wq_relay, h, sub)
            at(16.05 if stage == 0 and sub == 0 else 20.1 + 0.1 * h, wo_start, h, sub)
            at(((25.0, 26.15), (28.3, 30.42), (30.43, 30.6))[stage][sub], wo_pass, h, sub)
            at((30.9, 32.0, 34.1)[stage], wo_relay, h, sub)
        at((12.0, 16.0, 20.0)[stage], q_part, h)
        at((16.5, 20.1, 23.5)[stage], q_make, h, 0)
        at((16.6, 25.9, 30.2)[stage], kv_ready, h)
        at((16.7, 26.1, 30.5)[stage], att_own, h)
        at((21.9, 27.2, 30.4)[stage], att_mate, h)
        if h < last:
            at(34.05 if h < last - 1 else 37.5, project, h)
            at(24.5 if stage == 0 else 27.25, o_send, h, 0)
        at((31.0, 31.9, 33.2)[stage], merge, h, 0)
    at(23.6, q_make, last, 1)
    at(34.0, merge, last, 1)
    at(4.0, norm)
    at(16.45, factor)
    for when, order, step, args in sorted(events, key=lambda event: event[:2]):
        with jax.named_scope("_".join([step.__name__] + [str(a) for a in args])):
            step(*args)

    wo_ready(last)
    for b, (place, part) in enumerate(parts_of(last)):
        with jax.named_scope(f"tail_wait_{b}"):
            att_wait(last, b)
        for start in starts:
            cols = slice(start, start + tile)
            result = oacc[part, cols] + jnp.dot(
                att[part, last * span :],
                wo[last * span :, cols],
                preferred_element_type=jnp.float32,
            )
            out_ref[part, cols] = result.astype(jnp.bfloat16)
    with jax.named_scope("drain"):
        sent(kvbuf.at[:, 0:7], 0)
        if n_peer:
            sent(wq.at[0:n_peer], 1)
            sent(sqbuf.at[0:n_peer], 2)
            sent(qsend.at[0:n_peer], 3)
            sent(qsend.at[0:n_peer], 4)
            sent(wo.at[0 : n_peer * width], 8)
        if n_mate:
            sent(qmate.at[:, 0:n_mate], 5)
            sent(osend.at[:, 0:n_mate], 6)
            sent(ssend.at[:, 0:n_mate], 7)


def per_device(n_blk, n_tp, dec_states, norm_gain, query_weight, out_weight, enc_keys, enc_values):
    rows, feat = dec_states.shape
    width = query_weight.shape[1]
    enc_rows = enc_keys.shape[0]
    heads = width // HEAD_DIM
    n_pair = n_blk // 8
    bf16, f32 = jnp.bfloat16, jnp.float32
    dma = pltpu.SemaphoreType.DMA
    anywhere = pl.BlockSpec(memory_space=pl.ANY)
    return pl.pallas_call(
        functools.partial(kernel, n_blk, n_tp),
        out_shape=pltpu.VMEM((rows, feat), bf16),
        in_specs=[
            anywhere,
            anywhere,
            anywhere,
            anywhere,
            anywhere,
            anywhere,
        ],
        out_specs=pl.BlockSpec(memory_space=pltpu.VMEM),
        scratch_shapes=[
            pltpu.VMEM((1, n_tp * feat), f32),
            pltpu.VMEM((2 * heads, 8, enc_rows, HEAD_DIM), bf16),
            pltpu.VMEM((feat, width), bf16),
            pltpu.VMEM((n_tp, heads, feat, HEAD_DIM), bf16),
            pltpu.VMEM((n_tp * width, feat), bf16),
            pltpu.VMEM((rows, feat), bf16),
            pltpu.VMEM((rows, feat), bf16),
            pltpu.VMEM((n_tp, heads, rows, HEAD_DIM), bf16),
            pltpu.VMEM((n_tp, heads, rows, HEAD_DIM), bf16),
            pltpu.VMEM((rows, width), f32),
            pltpu.VMEM((n_tp, 8, rows), f32),
            pltpu.VMEM((rows, LANES), f32),
            pltpu.VMEM((heads, rows, HEAD_DIM), bf16),
            pltpu.VMEM((heads, n_pair, rows, HEAD_DIM), bf16),
            pltpu.VMEM((heads, n_pair, rows, HEAD_DIM), bf16),
            pltpu.VMEM((heads, n_pair, rows, HEAD_DIM), bf16),
            pltpu.VMEM((heads, n_pair, 1, rows), f32),
            pltpu.VMEM((heads, n_pair, 1, rows), f32),
            pltpu.VMEM((heads, rows, HEAD_DIM), f32),
            pltpu.VMEM((heads, rows, LANES), f32),
            pltpu.VMEM((rows, n_tp * width), bf16),
            pltpu.VMEM((rows, feat), f32),
            dma((9,)),
            dma((2 * heads, 3)),
            dma((heads,)),
            dma((n_tp - 1, heads, 2 * SUBS)),
            dma((n_tp - 1, heads)),
            dma((n_tp - 1, heads, 2 * SUBS)),
            dma((n_tp - 1, heads)),
            dma((n_tp - 1,)),
            dma((2, n_tp - 1, heads + 1)),
            dma((3, heads + 1, max(n_pair - 1, 1))),
            dma((heads,)),
            dma((4,)),
        ],
        compiler_params=pltpu.CompilerParams(
            collective_id=0, has_side_effects=True, vmem_limit_bytes=60 * 1024 * 1024
        ),
    )(dec_states, norm_gain.reshape(1, -1), query_weight, out_weight, enc_keys, enc_values)


def solution(mesh):
    in_specs = (P("blk", "tp"), P(), P(None, "tp"), P("tp", None), P("blk", "tp"), P("blk", "tp"))
    out_specs = P("blk", "tp")
    body = functools.partial(per_device, mesh.shape["blk"], mesh.shape["tp"])
    return jax.shard_map(body, mesh=mesh, in_specs=in_specs, out_specs=out_specs, check_vma=False)
```

```python
import functools
import math

import jax
import jax.numpy as jnp
from jax import lax
from jax.experimental import pallas as pl
from jax.experimental.pallas import tpu as pltpu
from jax.sharding import PartitionSpec as P

HEAD_DIM = 128
NORM_EPS = 1e-06
LANES = 128
SUBS = 2


def column_tile(width, limit=640):
    best = LANES
    for tile in range(LANES, limit + 1, LANES):
        if width % tile == 0:
            best = tile
    return best


def kernel(
    n_blk,
    n_tp,
    x_hbm,
    gain_hbm,
    wq_hbm,
    wo_hbm,
    k_hbm,
    v_hbm,
    out_ref,
    gain_ref,
    kvbuf,
    wq_own,
    wq,
    wo,
    xbuf,
    xg,
    qsend,
    qrecv,
    own_part,
    sqbuf,
    fbuf,
    qbuf,
    qmate,
    osend,
    orecv,
    ssend,
    srecv,
    opart,
    lse_own,
    att,
    oacc,
    send_sem,
    kv_recv,
    kv_core_recv,
    wq_recv,
    wq_core_recv,
    wo_recv,
    wo_core_recv,
    sq_recv,
    head_recv,
    mate_recv,
    kv_local,
    local_sem,
):
    n_line = n_blk // 4
    n_pair = n_line // 2
    b = lax.axis_index("blk")
    t = lax.axis_index("tp")
    core = lax.rem(b, 2)
    side = lax.rem(lax.div(b, 2), 2)
    line = lax.div(b, 4)
    par = lax.rem(line, 2)
    pair = lax.div(line, 2)
    rows = x_hbm.shape[0]
    feat = x_hbm.shape[1]
    width = wq_hbm.shape[1]
    heads = width // HEAD_DIM
    span = n_tp * HEAD_DIM
    last = heads - 1
    wq_rows = feat // (4 * SUBS)
    wo_rows = HEAD_DIM // (4 * SUBS)

    def index(zz, yy, cc):
        return (zz * 2 + yy) * 2 + cc

    sibling = index(line, side, 1 - core)
    beside = index(line, 1 - side, core)
    partner = index(line + 1 - 2 * par, side, core)
    peers = [lax.rem(t + off, n_tp) for off in range(1, n_tp)]
    mates = [lax.rem(pair + off, n_pair) for off in range(1, n_pair)]
    n_peer, n_mate = len(peers), len(mates)

    def mate_index(m):
        return index(2 * m + par, side, core)

    def parts_of(h):
        if h < last:
            return [(h, slice(0, rows))]
        return [(h, slice(0, rows // 2)), (h + 1, slice(rows // 2, rows))]

    def ds(start, size, mult=LANES):
        return pl.ds(pl.multiple_of(start, mult), size)

    def head_cols(h):
        return slice(h * HEAD_DIM, (h + 1) * HEAD_DIM)

    def slot(pp, yy, cc):
        return (pp * 2 + yy) * 2 + cc

    mine = slot(par, side, core)

    kv_loads = [
        pltpu.make_async_copy(
            (k_hbm, v_hbm)[e % 2].at[:, head_cols(e // 2)], kvbuf.at[e, mine], kv_local.at[e // 2]
        )
        for e in range(2 * heads)
    ]
    x_load = pltpu.make_async_copy(x_hbm, xbuf, local_sem.at[0])
    gain_load = pltpu.make_async_copy(gain_hbm, gain_ref, local_sem.at[3])
    wq_load = pltpu.make_async_copy(wq_hbm.at[ds(t * feat, feat)], wq_own, local_sem.at[1])
    wo_loads = [
        pltpu.make_async_copy(
            wo_hbm.at[head_cols(h), ds(t * feat, feat)],
            wo.at[ds(h * span + t * HEAD_DIM, HEAD_DIM)],
            local_sem.at[2],
        )
        for h in range(heads)
    ]
    for load in kv_loads[:2] + [gain_load, x_load, wq_load] + kv_loads[2:] + wo_loads:
        load.start()

    barrier = pltpu.get_barrier_semaphore()
    for other in [sibling, beside, partner] + [mate_index(m) for m in mates]:
        pl.semaphore_signal(barrier, inc=1, device_id={"blk": other})
    for p in peers:
        pl.semaphore_signal(barrier, inc=1, device_id={"tp": p})
    pl.semaphore_wait(barrier, 3 + len(mates) + len(peers))

    def remote(src, dst, kind, recv_sem, device_id):
        return pltpu.make_async_remote_copy(
            src_ref=src,
            dst_ref=dst,
            send_sem=send_sem.at[kind],
            recv_sem=recv_sem,
            device_id=device_id,
        )

    def arrived(ref, recv_sem):
        remote(ref, ref, 0, recv_sem, {"blk": sibling}).wait_recv()

    def sent(ref, kind):
        remote(ref, ref, kind, kv_core_recv.at[0], {"blk": sibling}).wait_send()

    def kv_send(e, s, kind, target):
        ref = kvbuf.at[e, s]
        remote(ref, ref, 0, kv_recv.at[e, kind], {"blk": target}).start()

    def kv_share(e, s):
        ref = kvbuf.at[e, s]
        remote(ref, ref, 0, kv_core_recv.at[e // 2], {"blk": sibling}).start()

    def kv_wait(e, s, kind):
        arrived(kvbuf.at[e, s], kv_recv.at[e, kind])

    from_beside = slot(par, 1 - side, core)
    from_partner = slot(1 - par, side, core)
    from_corner = slot(1 - par, 1 - side, core)

    def kv_loaded(h):
        both = kvbuf.at[2 * h : 2 * h + 2, mine]
        pltpu.make_async_copy(both, both, kv_local.at[h]).wait()

    def kv_line(e):
        kv_send(e, mine, 1, partner)

    def kv_side(e):
        kv_send(e, mine, 0, beside)

    def kv_core(e):
        kv_share(e, mine)

    def kv_from_partner(e):
        kv_wait(e, from_partner, 1)
        kv_send(e, from_partner, 2, beside)
        kv_share(e, from_partner)

    def kv_from_beside(e):
        kv_wait(e, from_beside, 0)
        kv_share(e, from_beside)

    def kv_from_corner(e):
        kv_wait(e, from_corner, 2)
        kv_share(e, from_corner)

    def kv_ready(h):
        arrived(kvbuf.at[2 * h : 2 * h + 2, 0:4], kv_core_recv.at[h])

    def wq_chunk(pp, cc, sub):
        return (pp * 2 + cc) * SUBS + sub

    def wq_ref(p, h, c):
        return wq.at[p, h, ds(c * wq_rows, wq_rows, 16)]

    def wq_hop(j, h, c, k):
        ref = wq_ref(peers[j], h, c)
        remote(ref, ref, 1, wq_recv.at[j, h, k], {"blk": partner}).start()

    def wq_share(j, h, c):
        ref = wq_ref(peers[j], h, c)
        remote(ref, ref, 1, wq_core_recv.at[j, h], {"blk": sibling}).start()

    def wq_start(h, k):
        for j, p in enumerate(peers):
            c = wq_chunk(par if k < SUBS else 1 - par, core, k % SUBS)
            src = wq_hbm.at[ds(p * feat + c * wq_rows, wq_rows, 16), head_cols(h)]
            place = wq_recv.at[n_peer - 1 - j, h, k]
            remote(src, wq_ref(t, h, c), 1, place, {"tp": p}).start()

    def wq_pass(h, sub):
        for j, p in enumerate(peers):
            c = wq_chunk(par, core, sub)
            arrived(wq_ref(p, h, c), wq_recv.at[j, h, sub])
            if h != last:
                wq_hop(j, h, c, SUBS + sub)
            wq_share(j, h, c)

    def wq_relay(h, sub):
        for j, p in enumerate(peers):
            c = wq_chunk(1 - par, core, sub)
            arrived(wq_ref(p, h, c), wq_recv.at[j, h, SUBS + sub])
            wq_share(j, h, c)

    def q_part(h):
        for j, p in enumerate(peers):
            arrived(wq.at[p, h, 0 : feat // 2], wq_core_recv.at[j, h])
            qsend[p, h] = jnp.dot(
                xg[...], wq[p, h], preferred_element_type=jnp.float32
            ).astype(jnp.bfloat16)
            for place, part in parts_of(h):
                remote(
                    qsend.at[p, h, part],
                    qrecv.at[t, h, part],
                    3,
                    head_recv.at[0, n_peer - 1 - j, place],
                    {"tp": p},
                ).start()

    tile = column_tile(feat)

    def norm():
        gain_load.wait()
        x_load.wait()
        squares = jnp.zeros((rows, 1), jnp.float32)
        for start in range(0, feat, tile):
            piece = xbuf[:, start : start + tile].astype(jnp.float32)
            squares += jnp.sum(piece * piece, axis=1, keepdims=True)
            gain = gain_ref[:, ds(t * feat + start, tile)]
            xg[:, start : start + tile] = (piece * gain).astype(jnp.bfloat16)
        wide = jnp.broadcast_to(squares, (rows, LANES))
        sqbuf[t] = jnp.transpose(wide)[0:8, :]
        for j, p in enumerate(peers):
            ref = sqbuf.at[t]
            remote(ref, ref, 2, sq_recv.at[n_peer - 1 - j], {"tp": p}).start()
        wq_load.wait()
        own_part[...] = jnp.dot(xg[...], wq_own[...], preferred_element_type=jnp.float32)

    def factor():
        total = sqbuf[t][0:1, :]
        for j, p in enumerate(peers):
            arrived(sqbuf.at[p], sq_recv.at[j])
            total = total + sqbuf[p][0:1, :]
        column = jnp.transpose(jnp.broadcast_to(total, (LANES, rows)))
        scale = math.log2(math.e) / math.sqrt(HEAD_DIM)
        fbuf[...] = lax.rsqrt(column / (feat * n_tp) + NORM_EPS) * scale

    def mate_send(k, src, dst, place, i):
        there = mate_recv.at[k, place, n_mate - 1 - i]
        remote(src, dst, 5 + k, there, {"blk": mate_index(mates[i])}).start()

    def q_make(h, b):
        place, part = parts_of(h)[b]
        summed = own_part[part, head_cols(h)]
        for j, p in enumerate(peers):
            arrived(qrecv.at[p, h, part], head_recv.at[0, j, place])
            summed = summed + qrecv[p, h, part].astype(jnp.float32)
        qbuf[h, part] = (summed * fbuf[part]).astype(jnp.bfloat16)
        for i in range(n_mate):
            mate_send(0, qbuf.at[h, part], qmate.at[h, pair, part], place, i)

    def attend(h, query, emit):
        half = rows // 2

        def score(b):
            block = query(b, slice(b * half, b * half + half))
            scores = []
            for i in range(4):
                keys = kvbuf[2 * h, 2 * i : 2 * i + 2].reshape(-1, HEAD_DIM)
                scores.append(
                    lax.dot_general(
                        block, keys, (((1,), (1,)), ((), ())), preferred_element_type=jnp.float32
                    )
                )
            return scores

        later = score(0)
        for b in range(2):
            scores = later
            if b == 0:
                later = score(1)
            top = scores[0]
            for s in scores[1:]:
                top = jnp.maximum(top, s)
            top = jnp.max(top, axis=1, keepdims=True)
            mixed = jnp.zeros((half, 2 * HEAD_DIM), jnp.float32)
            for i in range(4):
                vals = kvbuf[2 * h + 1, 2 * i : 2 * i + 2].reshape(-1, HEAD_DIM)
                wide = jnp.concatenate([vals, jnp.ones_like(vals)], axis=1)
                weights = jnp.exp2(scores[i] - top).astype(jnp.bfloat16)
                mixed = mixed + jnp.dot(weights, wide, preferred_element_type=jnp.float32)
            total = mixed[:, HEAD_DIM:]
            lse = top + jnp.log(total) * math.log2(math.e)
            emit(b, slice(b * half, b * half + half), mixed[:, :HEAD_DIM] / total, lse)

    def att_own(h):
        def emit(b, part, out, lse):
            opart[h, part] = out
            lse_own[h, part] = lse

        attend(h, lambda b, part: qbuf[h, part], emit)

    def o_send(h, b):
        place, part = parts_of(h)[b]
        for i, m in enumerate(mates):
            mate_send(1, osend.at[h, m, part], orecv.at[h, pair, part], place, i)
            here, there = ssend.at[h, m, :, part], srecv.at[h, pair, :, part]
            mate_send(2, here, there, place, i)

    def att_mate(h):
        for i, m in enumerate(mates):

            def query(b, part):
                if b < len(parts_of(h)):
                    place, piece = parts_of(h)[b]
                    arrived(qmate.at[h, m, piece], mate_recv.at[0, place, i])
                return qmate[h, m, part]

            def emit(b, part, out, lse):
                osend[h, m, part] = out.astype(jnp.bfloat16)
                ssend[h, m, :, part] = jnp.transpose(lse)[0:1, :]

            attend(h, query, emit)

    def att_ref(p, h, part):
        return att.at[part, ds(h * span + p * HEAD_DIM, HEAD_DIM)]

    def merge(h, b):
        place, part = parts_of(h)[b]
        parts = [opart[h, part]]
        logs = [lse_own[h, part]]
        for i, m in enumerate(mates):
            arrived(srecv.at[h, m, :, part], mate_recv.at[2, place, i])
            arrived(orecv.at[h, m, part], mate_recv.at[1, place, i])
            parts.append(orecv[h, m, part].astype(jnp.float32))
            stat = srecv[h, m, :, part]
            logs.append(jnp.transpose(jnp.broadcast_to(stat, (LANES, stat.shape[1]))))
        top = logs[0]
        for log in logs[1:]:
            top = jnp.maximum(top, log)
        shares = [jnp.exp2(log - top) for log in logs]
        total = shares[0]
        mixed = shares[0] * parts[0]
        for share, piece in zip(shares[1:], parts[1:]):
            total = total + share
            mixed = mixed + share * piece
        att[part, ds(h * span + t * HEAD_DIM, HEAD_DIM)] = (mixed / total).astype(jnp.bfloat16)
        for j, p in enumerate(peers):
            there = head_recv.at[1, n_peer - 1 - j, place]
            remote(att_ref(t, h, part), att_ref(t, h, part), 4, there, {"tp": p}).start()

    def att_wait(h, b):
        place, part = parts_of(h)[b]
        for j, p in enumerate(peers):
            arrived(att_ref(p, h, part), head_recv.at[1, j, place])

    def wo_ref(p, h, q):
        return wo.at[ds(h * span + p * HEAD_DIM + q * wo_rows, wo_rows, wo_rows)]

    def wo_chunk(yy, cc, sub):
        return (yy * 2 + cc) * SUBS + sub

    def wo_start(h, k):
        q = wo_chunk(side if k < SUBS else 1 - side, core, k % SUBS)
        for j, p in enumerate(peers):
            src = wo_hbm.at[ds(h * HEAD_DIM + q * wo_rows, wo_rows, wo_rows), ds(p * feat, feat)]
            place = wo_recv.at[n_peer - 1 - j, h, k]
            remote(src, wo_ref(t, h, q), 8, place, {"tp": p}).start()

    def wo_pass(h, sub):
        for j, p in enumerate(peers):
            ref = wo_ref(p, h, wo_chunk(side, core, sub))
            arrived(ref, wo_recv.at[j, h, sub])
            if h != last:
                remote(ref, ref, 8, wo_recv.at[j, h, SUBS + sub], {"blk": beside}).start()
            remote(ref, ref, 8, wo_core_recv.at[j, h], {"blk": sibling}).start()

    def wo_relay(h, sub):
        for j, p in enumerate(peers):
            ref = wo_ref(p, h, wo_chunk(1 - side, core, sub))
            arrived(ref, wo_recv.at[j, h, SUBS + sub])
            remote(ref, ref, 8, wo_core_recv.at[j, h], {"blk": sibling}).start()

    def wo_loaded():
        ref = wo.at[0:width]
        pltpu.make_async_copy(ref, ref, local_sem.at[2]).wait()

    def wo_ready(h):
        for j in range(n_peer):
            arrived(wo.at[0 : HEAD_DIM // 2], wo_core_recv.at[j, h])

    starts = range(0, feat, tile)

    def project(h):
        if h == 0:
            wo_loaded()
        wo_ready(h)
        att_wait(h, 0)
        for start in starts:
            cols = slice(start, start + tile)
            block = slice(h * span, (h + 1) * span)
            result = jnp.dot(att[:, block], wo[block, cols], preferred_element_type=jnp.float32)
            oacc[:, cols] = result if h == 0 else oacc[:, cols] + result

    events = []

    def at(when, step, *args):
        events.append((when, len(events), step, args))

    for h in range(heads):
        k, v = 2 * h, 2 * h + 1
        stage = max(h - last + 2, 0)
        for piece in range(2 * SUBS if h == last else SUBS):
            at(12.01 if piece >= 2 * SUBS - 1 else 2.0 + 0.1 * h, wq_start, h, piece)
        at(2.45 if h == 0 else 2.6 + 0.01 * h, kv_loaded, h)
        for e in (k, v):
            at((2.5 + 0.01 * e, 9.36, 14.25 if e == k else 16.55)[stage], kv_line, e)
            at((2.5 + 0.01 * e, 2.65, 7.05)[stage], kv_side, e)
            at(2.7 + 0.01 * e, kv_core, e)
        at((4.9, 16.2, 21.85)[stage], kv_from_partner, k)
        at((7.0, 18.1, 24.6)[stage], kv_from_partner, v)
        at((7.1, 9.4, 20.2)[stage], kv_from_beside, k)
        at((7.2, 10.8, 20.3)[stage], kv_from_beside, v)
        at((12.6, 22.6, 27.1)[stage], kv_from_corner, k)
        at((14.6, 24.7, 28.2)[stage], kv_from_corner, v)
        for piece in range(2 * SUBS if h == last else SUBS):
            at(16.05 if stage == 0 else 20.1 + 0.1 * h, wo_start, h, piece)
        for sub in range(SUBS):
            at((4.2, 7.6, 11.2)[stage] + 1.75 * sub, wq_pass, h, sub)
            at((10.2, 14.2, 15.2)[stage] + (3.3 if h == last else 0.1) * sub, wq_relay, h, sub)
            at(((25.0, 26.15), (28.25, 28.3), (30.43, 30.6))[stage][sub], wo_pass, h, sub)
            at((30.9, 34.03, 34.2)[stage], wo_relay, h, sub)
        at((12.0, 16.0, 20.0)[stage], q_part, h)
        at((15.5, 20.1, 23.5)[stage], q_make, h, 0)
        at((16.6, 25.9, 30.2)[stage], kv_ready, h)
        at((16.7, 26.1, 30.5)[stage], att_own, h)
        at((21.9, 27.2, 30.4)[stage], att_mate, h)
        if h < last:
            at(34.05 if h < last - 1 else 37.5, project, h)
        for b in range(len(parts_of(h))):
            at((24.5, 27.25, 30.4)[stage], o_send, h, b)
        at((31.0, 31.9, 33.2)[stage], merge, h, 0)
    at(23.6, q_make, last, 1)
    at(34.0, merge, last, 1)
    at(4.0, norm)
    at(15.45, factor)
    for when, order, step, args in sorted(events, key=lambda event: event[:2]):
        with jax.named_scope("_".join([step.__name__] + [str(a) for a in args])):
            step(*args)

    wo_ready(last)
    for b, (place, part) in enumerate(parts_of(last)):
        with jax.named_scope(f"tail_wait_{b}"):
            att_wait(last, b)
        for start in starts:
            cols = slice(start, start + tile)
            result = oacc[part, cols] + jnp.dot(
                att[part, last * span :],
                wo[last * span :, cols],
                preferred_element_type=jnp.float32,
            )
            out_ref[part, cols] = result.astype(jnp.bfloat16)
    with jax.named_scope("drain"):
        sent(kvbuf.at[:, 0:7], 0)
        if n_peer:
            sent(wq.at[0:n_peer], 1)
            sent(sqbuf.at[0:n_peer], 2)
            sent(qsend.at[0:n_peer], 3)
            sent(qsend.at[0:n_peer], 4)
            sent(wo.at[0 : n_peer * width], 8)
        if n_mate:
            sent(qmate.at[:, 0:n_mate], 5)
            sent(osend.at[:, 0:n_mate], 6)
            sent(ssend.at[:, 0:n_mate], 7)


def per_device(n_blk, n_tp, dec_states, norm_gain, query_weight, out_weight, enc_keys, enc_values):
    rows, feat = dec_states.shape
    width = query_weight.shape[1]
    enc_rows = enc_keys.shape[0]
    heads = width // HEAD_DIM
    n_pair = n_blk // 8
    bf16, f32 = jnp.bfloat16, jnp.float32
    dma = pltpu.SemaphoreType.DMA
    anywhere = pl.BlockSpec(memory_space=pl.ANY)
    return pl.pallas_call(
        functools.partial(kernel, n_blk, n_tp),
        out_shape=pltpu.VMEM((rows, feat), bf16),
        in_specs=[
            anywhere,
            anywhere,
            anywhere,
            anywhere,
            anywhere,
            anywhere,
        ],
        out_specs=pl.BlockSpec(memory_space=pltpu.VMEM),
        scratch_shapes=[
            pltpu.VMEM((1, n_tp * feat), f32),
            pltpu.VMEM((2 * heads, 8, enc_rows, HEAD_DIM), bf16),
            pltpu.VMEM((feat, width), bf16),
            pltpu.VMEM((n_tp, heads, feat, HEAD_DIM), bf16),
            pltpu.VMEM((n_tp * width, feat), bf16),
            pltpu.VMEM((rows, feat), bf16),
            pltpu.VMEM((rows, feat), bf16),
            pltpu.VMEM((n_tp, heads, rows, HEAD_DIM), bf16),
            pltpu.VMEM((n_tp, heads, rows, HEAD_DIM), bf16),
            pltpu.VMEM((rows, width), f32),
            pltpu.VMEM((n_tp, 8, rows), f32),
            pltpu.VMEM((rows, LANES), f32),
            pltpu.VMEM((heads, rows, HEAD_DIM), bf16),
            pltpu.VMEM((heads, n_pair, rows, HEAD_DIM), bf16),
            pltpu.VMEM((heads, n_pair, rows, HEAD_DIM), bf16),
            pltpu.VMEM((heads, n_pair, rows, HEAD_DIM), bf16),
            pltpu.VMEM((heads, n_pair, 1, rows), f32),
            pltpu.VMEM((heads, n_pair, 1, rows), f32),
            pltpu.VMEM((heads, rows, HEAD_DIM), f32),
            pltpu.VMEM((heads, rows, LANES), f32),
            pltpu.VMEM((rows, n_tp * width), bf16),
            pltpu.VMEM((rows, feat), f32),
            dma((9,)),
            dma((2 * heads, 3)),
            dma((heads,)),
            dma((n_tp - 1, heads, 2 * SUBS)),
            dma((n_tp - 1, heads)),
            dma((n_tp - 1, heads, 2 * SUBS)),
            dma((n_tp - 1, heads)),
            dma((n_tp - 1,)),
            dma((2, n_tp - 1, heads + 1)),
            dma((3, heads + 1, max(n_pair - 1, 1))),
            dma((heads,)),
            dma((4,)),
        ],
        compiler_params=pltpu.CompilerParams(
            collective_id=0, has_side_effects=True, vmem_limit_bytes=60 * 1024 * 1024
        ),
    )(dec_states, norm_gain.reshape(1, -1), query_weight, out_weight, enc_keys, enc_values)


def solution(mesh):
    in_specs = (P("blk", "tp"), P(), P(None, "tp"), P("tp", None), P("blk", "tp"), P("blk", "tp"))
    out_specs = P("blk", "tp")
    body = functools.partial(per_device, mesh.shape["blk"], mesh.shape["tp"])
    return jax.shard_map(body, mesh=mesh, in_specs=in_specs, out_specs=out_specs, check_vma=False)
```

```python
import functools
import math

import jax
import jax.numpy as jnp
from jax import lax
from jax.experimental import pallas as pl
from jax.experimental.pallas import tpu as pltpu
from jax.sharding import PartitionSpec as P

HEAD_DIM = 128
NORM_EPS = 1e-06
LANES = 128
SUBS = 2


def column_tile(width, limit=640):
    best = LANES
    for tile in range(LANES, limit + 1, LANES):
        if width % tile == 0:
            best = tile
    return best


def kernel(
    n_blk,
    n_tp,
    x_hbm,
    gain_hbm,
    wq_hbm,
    wo_hbm,
    k_hbm,
    v_hbm,
    out_ref,
    gain_ref,
    kvbuf,
    wq_own,
    wq,
    wo,
    xbuf,
    xg,
    qsend,
    qrecv,
    own_part,
    sqbuf,
    fbuf,
    qbuf,
    qmate,
    osend,
    orecv,
    ssend,
    srecv,
    opart,
    lse_own,
    att,
    oacc,
    send_sem,
    kv_recv,
    kv_core_recv,
    wq_recv,
    wq_core_recv,
    sq_recv,
    head_recv,
    mate_recv,
    kv_local,
    local_sem,
):
    n_line = n_blk // 4
    n_pair = n_line // 2
    b = lax.axis_index("blk")
    t = lax.axis_index("tp")
    core = lax.rem(b, 2)
    side = lax.rem(lax.div(b, 2), 2)
    line = lax.div(b, 4)
    par = lax.rem(line, 2)
    pair = lax.div(line, 2)
    rows = x_hbm.shape[0]
    feat = x_hbm.shape[1]
    width = wq_hbm.shape[1]
    heads = width // HEAD_DIM
    span = n_tp * HEAD_DIM
    last = heads - 1
    wq_rows = feat // (4 * SUBS)
    wo_rows = HEAD_DIM // (4 * SUBS)

    def index(zz, yy, cc):
        return (zz * 2 + yy) * 2 + cc

    sibling = index(line, side, 1 - core)
    beside = index(line, 1 - side, core)
    partner = index(line + 1 - 2 * par, side, core)
    peers = [lax.rem(t + off, n_tp) for off in range(1, n_tp)]
    mates = [lax.rem(pair + off, n_pair) for off in range(1, n_pair)]
    n_peer, n_mate = len(peers), len(mates)

    def mate_index(m):
        return index(2 * m + par, side, core)

    def parts_of(h):
        if h < last:
            return [(h, slice(0, rows))]
        return [(h, slice(0, rows // 2)), (h + 1, slice(rows // 2, rows))]

    def ds(start, size, mult=LANES):
        return pl.ds(pl.multiple_of(start, mult), size)

    def head_cols(h):
        return slice(h * HEAD_DIM, (h + 1) * HEAD_DIM)

    def slot(pp, yy, cc):
        return (pp * 2 + yy) * 2 + cc

    mine = slot(par, side, core)

    kv_loads = [
        pltpu.make_async_copy(
            (k_hbm, v_hbm)[e % 2].at[:, head_cols(e // 2)], kvbuf.at[e, mine], kv_local.at[e // 2]
        )
        for e in range(2 * heads)
    ]
    x_load = pltpu.make_async_copy(x_hbm, xbuf, local_sem.at[0])
    gain_load = pltpu.make_async_copy(gain_hbm, gain_ref, local_sem.at[3])
    wq_load = pltpu.make_async_copy(wq_hbm.at[ds(t * feat, feat)], wq_own, local_sem.at[1])
    wo_loads = [
        pltpu.make_async_copy(
            wo_hbm.at[head_cols(h), ds(t * feat, feat)],
            wo.at[ds(h * span + t * HEAD_DIM, HEAD_DIM)],
            local_sem.at[2],
        )
        for h in range(heads)
    ]
    for load in kv_loads[:2] + [gain_load, x_load, wq_load] + kv_loads[2:] + wo_loads:
        load.start()

    barrier = pltpu.get_barrier_semaphore()
    for other in [sibling, beside, partner] + [mate_index(m) for m in mates]:
        pl.semaphore_signal(barrier, inc=1, device_id={"blk": other})
    for p in peers:
        pl.semaphore_signal(barrier, inc=1, device_id={"tp": p})
    pl.semaphore_wait(barrier, 3 + len(mates) + len(peers))

    def remote(src, dst, kind, recv_sem, device_id):
        return pltpu.make_async_remote_copy(
            src_ref=src,
            dst_ref=dst,
            send_sem=send_sem.at[kind],
            recv_sem=recv_sem,
            device_id=device_id,
        )

    def arrived(ref, recv_sem):
        remote(ref, ref, 0, recv_sem, {"blk": sibling}).wait_recv()

    def sent(ref, kind):
        remote(ref, ref, kind, kv_core_recv.at[0], {"blk": sibling}).wait_send()

    def kv_send(e, s, kind, target):
        ref = kvbuf.at[e, s]
        remote(ref, ref, 0, kv_recv.at[e, kind], {"blk": target}).start()

    def kv_share(e, s):
        ref = kvbuf.at[e, s]
        remote(ref, ref, 0, kv_core_recv.at[e // 2], {"blk": sibling}).start()

    def kv_wait(e, s, kind):
        arrived(kvbuf.at[e, s], kv_recv.at[e, kind])

    from_beside = slot(par, 1 - side, core)
    from_partner = slot(1 - par, side, core)
    from_corner = slot(1 - par, 1 - side, core)

    def kv_loaded(h):
        both = kvbuf.at[2 * h : 2 * h + 2, mine]
        pltpu.make_async_copy(both, both, kv_local.at[h]).wait()

    def kv_line(e):
        kv_send(e, mine, 1, partner)

    def kv_side(e):
        kv_send(e, mine, 0, beside)

    def kv_core(e):
        kv_share(e, mine)

    def kv_from_partner(e):
        kv_wait(e, from_partner, 1)
        kv_send(e, from_partner, 2, beside)
        kv_share(e, from_partner)

    def kv_from_beside(e):
        kv_wait(e, from_beside, 0)
        kv_share(e, from_beside)

    def kv_from_corner(e):
        kv_wait(e, from_corner, 2)
        kv_share(e, from_corner)

    def kv_ready(h):
        arrived(kvbuf.at[2 * h : 2 * h + 2, 0:4], kv_core_recv.at[h])

    def wq_chunk(pp, cc, sub):
        return (pp * 2 + cc) * SUBS + sub

    def wq_ref(p, h, c):
        return wq.at[p, h, ds(c * wq_rows, wq_rows, 16)]

    def wq_hop(j, h, c, k):
        ref = wq_ref(peers[j], h, c)
        remote(ref, ref, 1, wq_recv.at[j, h, k], {"blk": partner}).start()

    def wq_share(j, h, c):
        ref = wq_ref(peers[j], h, c)
        remote(ref, ref, 1, wq_core_recv.at[j, h], {"blk": sibling}).start()

    def wq_start(h, k):
        for j, p in enumerate(peers):
            c = wq_chunk(par if k < SUBS else 1 - par, core, k % SUBS)
            src = wq_hbm.at[ds(p * feat + c * wq_rows, wq_rows, 16), head_cols(h)]
            place = wq_recv.at[n_peer - 1 - j, h, k]
            remote(src, wq_ref(t, h, c), 1, place, {"tp": p}).start()

    def wq_pass(h, sub):
        for j, p in enumerate(peers):
            c = wq_chunk(par, core, sub)
            arrived(wq_ref(p, h, c), wq_recv.at[j, h, sub])
            if h != last:
                wq_hop(j, h, c, SUBS + sub)
            wq_share(j, h, c)

    def wq_relay(h, sub):
        for j, p in enumerate(peers):
            c = wq_chunk(1 - par, core, sub)
            arrived(wq_ref(p, h, c), wq_recv.at[j, h, SUBS + sub])
            wq_share(j, h, c)

    def q_part(h):
        for j, p in enumerate(peers):
            arrived(wq.at[p, h, 0 : feat // 2], wq_core_recv.at[j, h])
            qsend[p, h] = jnp.dot(
                xg[...], wq[p, h], preferred_element_type=jnp.float32
            ).astype(jnp.bfloat16)
            for place, part in parts_of(h):
                remote(
                    qsend.at[p, h, part],
                    qrecv.at[t, h, part],
                    3,
                    head_recv.at[0, n_peer - 1 - j, place],
                    {"tp": p},
                ).start()

    tile = column_tile(feat)

    def norm():
        gain_load.wait()
        x_load.wait()
        squares = jnp.zeros((rows, 1), jnp.float32)
        for start in range(0, feat, tile):
            piece = xbuf[:, start : start + tile].astype(jnp.float32)
            squares += jnp.sum(piece * piece, axis=1, keepdims=True)
            gain = gain_ref[:, ds(t * feat + start, tile)]
            xg[:, start : start + tile] = (piece * gain).astype(jnp.bfloat16)
        wide = jnp.broadcast_to(squares, (rows, LANES))
        sqbuf[t] = jnp.transpose(wide)[0:8, :]
        for j, p in enumerate(peers):
            ref = sqbuf.at[t]
            remote(ref, ref, 2, sq_recv.at[n_peer - 1 - j], {"tp": p}).start()
        wq_load.wait()
        own_part[...] = jnp.dot(xg[...], wq_own[...], preferred_element_type=jnp.float32)

    def factor():
        total = sqbuf[t][0:1, :]
        for j, p in enumerate(peers):
            arrived(sqbuf.at[p], sq_recv.at[j])
            total = total + sqbuf[p][0:1, :]
        column = jnp.transpose(jnp.broadcast_to(total, (LANES, rows)))
        scale = math.log2(math.e) / math.sqrt(HEAD_DIM)
        fbuf[...] = lax.rsqrt(column / (feat * n_tp) + NORM_EPS) * scale

    def mate_send(k, src, dst, place, i):
        there = mate_recv.at[k, place, n_mate - 1 - i]
        remote(src, dst, 5 + k, there, {"blk": mate_index(mates[i])}).start()

    def q_make(h, b):
        place, part = parts_of(h)[b]
        summed = own_part[part, head_cols(h)]
        for j, p in enumerate(peers):
            arrived(qrecv.at[p, h, part], head_recv.at[0, j, place])
            summed = summed + qrecv[p, h, part].astype(jnp.float32)
        qbuf[h, part] = (summed * fbuf[part]).astype(jnp.bfloat16)
        for i in range(n_mate):
            mate_send(0, qbuf.at[h, part], qmate.at[h, pair, part], place, i)

    def attend(h, query, emit):
        half = rows // 2

        def score(b):
            block = query(b, slice(b * half, b * half + half))
            scores = []
            for i in range(4):
                keys = kvbuf[2 * h, 2 * i : 2 * i + 2].reshape(-1, HEAD_DIM)
                scores.append(
                    lax.dot_general(
                        block, keys, (((1,), (1,)), ((), ())), preferred_element_type=jnp.float32
                    )
                )
            return scores

        later = score(0)
        for b in range(2):
            scores = later
            if b == 0:
                later = score(1)
            top = scores[0]
            for s in scores[1:]:
                top = jnp.maximum(top, s)
            top = jnp.max(top, axis=1, keepdims=True)
            mixed = jnp.zeros((half, 2 * HEAD_DIM), jnp.float32)
            for i in range(4):
                vals = kvbuf[2 * h + 1, 2 * i : 2 * i + 2].reshape(-1, HEAD_DIM)
                wide = jnp.concatenate([vals, jnp.ones_like(vals)], axis=1)
                weights = jnp.exp2(scores[i] - top).astype(jnp.bfloat16)
                mixed = mixed + jnp.dot(weights, wide, preferred_element_type=jnp.float32)
            total = mixed[:, HEAD_DIM:]
            lse = top + jnp.log(total) * math.log2(math.e)
            emit(b, slice(b * half, b * half + half), mixed[:, :HEAD_DIM] / total, lse)

    def att_own(h):
        def emit(b, part, out, lse):
            opart[h, part] = out
            lse_own[h, part] = lse

        attend(h, lambda b, part: qbuf[h, part], emit)

    def o_send(h, b):
        place, part = parts_of(h)[b]
        for i, m in enumerate(mates):
            mate_send(1, osend.at[h, m, part], orecv.at[h, pair, part], place, i)
            here, there = ssend.at[h, m, :, part], srecv.at[h, pair, :, part]
            mate_send(2, here, there, place, i)

    def att_mate(h):
        for i, m in enumerate(mates):

            def query(b, part):
                if b < len(parts_of(h)):
                    place, piece = parts_of(h)[b]
                    arrived(qmate.at[h, m, piece], mate_recv.at[0, place, i])
                return qmate[h, m, part]

            def emit(b, part, out, lse):
                osend[h, m, part] = out.astype(jnp.bfloat16)
                ssend[h, m, :, part] = jnp.transpose(lse)[0:1, :]

            attend(h, query, emit)

    def att_ref(p, h, part):
        return att.at[part, ds(h * span + p * HEAD_DIM, HEAD_DIM)]

    def merge(h, b):
        place, part = parts_of(h)[b]
        parts = [opart[h, part]]
        logs = [lse_own[h, part]]
        for i, m in enumerate(mates):
            arrived(srecv.at[h, m, :, part], mate_recv.at[2, place, i])
            arrived(orecv.at[h, m, part], mate_recv.at[1, place, i])
            parts.append(orecv[h, m, part].astype(jnp.float32))
            stat = srecv[h, m, :, part]
            logs.append(jnp.transpose(jnp.broadcast_to(stat, (LANES, stat.shape[1]))))
        top = logs[0]
        for log in logs[1:]:
            top = jnp.maximum(top, log)
        shares = [jnp.exp2(log - top) for log in logs]
        total = shares[0]
        mixed = shares[0] * parts[0]
        for share, piece in zip(shares[1:], parts[1:]):
            total = total + share
            mixed = mixed + share * piece
        att[part, ds(h * span + t * HEAD_DIM, HEAD_DIM)] = (mixed / total).astype(jnp.bfloat16)
        for j, p in enumerate(peers):
            there = head_recv.at[1, n_peer - 1 - j, place]
            remote(att_ref(t, h, part), att_ref(t, h, part), 4, there, {"tp": p}).start()

    def att_wait(h, b):
        place, part = parts_of(h)[b]
        for j, p in enumerate(peers):
            arrived(att_ref(p, h, part), head_recv.at[1, j, place])

    def wo_ref(p, h, q):
        return wo.at[ds(h * span + p * HEAD_DIM + q * wo_rows, wo_rows, wo_rows)]

    def wo_chunk(yy, cc, sub):
        return (yy * 2 + cc) * SUBS + sub

    def wo_start(h, k):
        q = wo_chunk(side if k < SUBS else 1 - side, core, k % SUBS)
        for j, p in enumerate(peers):
            src = wo_hbm.at[ds(h * HEAD_DIM + q * wo_rows, wo_rows, wo_rows), ds(p * feat, feat)]
            place = wq_recv.at[n_peer - 1 - j, h, k]
            remote(src, wo_ref(t, h, q), 8, place, {"tp": p}).start()

    def wo_pass(h, sub):
        for j, p in enumerate(peers):
            ref = wo_ref(p, h, wo_chunk(side, core, sub))
            arrived(ref, wq_recv.at[j, h, sub])
            if h != last or sub == 0:
                remote(ref, ref, 8, wq_recv.at[j, h, SUBS + sub], {"blk": beside}).start()
            remote(ref, ref, 8, wq_core_recv.at[j, h], {"blk": sibling}).start()

    def wo_relay(h, sub):
        for j, p in enumerate(peers):
            ref = wo_ref(p, h, wo_chunk(1 - side, core, sub))
            arrived(ref, wq_recv.at[j, h, SUBS + sub])
            remote(ref, ref, 8, wq_core_recv.at[j, h], {"blk": sibling}).start()

    def wo_loaded():
        ref = wo.at[0:width]
        pltpu.make_async_copy(ref, ref, local_sem.at[2]).wait()

    def wo_ready(h):
        for j in range(n_peer):
            arrived(wo.at[0 : HEAD_DIM // 2], wq_core_recv.at[j, h])

    starts = range(0, feat, tile)

    def project(h):
        if h == 0:
            wo_loaded()
        wo_ready(h)
        att_wait(h, 0)
        for start in starts:
            cols = slice(start, start + tile)
            block = slice(h * span, (h + 1) * span)
            result = jnp.dot(att[:, block], wo[block, cols], preferred_element_type=jnp.float32)
            oacc[:, cols] = result if h == 0 else oacc[:, cols] + result

    events = []

    def at(when, step, *args):
        events.append((when, len(events), step, args))

    for h in range(heads):
        k, v = 2 * h, 2 * h + 1
        stage = max(h - last + 2, 0)
        for piece in range(2 * SUBS if h == last else SUBS):
            at(12.01 if piece >= 2 * SUBS - 1 else 2.0 + 0.1 * h, wq_start, h, piece)
        at(2.45 if h == 0 else 2.6 + 0.01 * h, kv_loaded, h)
        for e in (k, v):
            at((2.5 + 0.01 * e, 9.36, 14.25 if e == k else 16.55)[stage], kv_line, e)
            at((2.5 + 0.01 * e, 2.65, 7.05)[stage], kv_side, e)
            at(2.7 + 0.01 * e, kv_core, e)
        at((4.9, 16.2, 21.85)[stage], kv_from_partner, k)
        at((7.0, 18.1, 24.6)[stage], kv_from_partner, v)
        at((7.1, 9.4, 20.2)[stage], kv_from_beside, k)
        at((7.2, 10.8, 20.3)[stage], kv_from_beside, v)
        at((12.6, 22.6, 27.1)[stage], kv_from_corner, k)
        at((14.6, 24.7, 28.2)[stage], kv_from_corner, v)
        for piece in range(2 * SUBS if h == last else SUBS):
            if piece != SUBS:
                at((16.05, 20.2, 23.65)[stage], wo_start, h, piece)
        for sub in range(SUBS):
            at((4.2, 7.6, 11.2)[stage] + 1.75 * sub, wq_pass, h, sub)
            at((10.2, 14.2, 15.2)[stage] + (3.3 if h == last else 0.1) * sub, wq_relay, h, sub)
            at(((25.0, 26.15), (28.25, 28.3), (30.43, 30.6))[stage][sub], wo_pass, h, sub)
            at((30.9, 34.03, 34.2)[stage], wo_relay, h, sub)
        at((12.0, 16.0, 20.0)[stage], q_part, h)
        at((15.5, 20.1, 23.5)[stage], q_make, h, 0)
        at((16.6, 25.9, 30.2)[stage], kv_ready, h)
        at((16.7, 26.1, 30.5)[stage], att_own, h)
        at((21.9, 27.2, 30.4)[stage], att_mate, h)
        if h < last:
            at(34.05 if h < last - 1 else 37.5, project, h)
        for b in range(len(parts_of(h))):
            at((24.5, 27.25, 30.4)[stage], o_send, h, b)
        at((31.0, 31.9, 33.2)[stage], merge, h, 0)
    at(23.6, q_make, last, 1)
    at(34.0, merge, last, 1)
    at(4.0, norm)
    at(15.45, factor)
    for when, order, step, args in sorted(events, key=lambda event: event[:2]):
        with jax.named_scope("_".join([step.__name__] + [str(a) for a in args])):
            step(*args)

    wo_ready(last)
    for b, (place, part) in enumerate(parts_of(last)):
        with jax.named_scope(f"tail_wait_{b}"):
            att_wait(last, b)
        for start in starts:
            cols = slice(start, start + tile)
            result = oacc[part, cols] + jnp.dot(
                att[part, last * span :],
                wo[last * span :, cols],
                preferred_element_type=jnp.float32,
            )
            out_ref[part, cols] = result.astype(jnp.bfloat16)
    with jax.named_scope("drain"):
        sent(kvbuf.at[:, 0:7], 0)
        if n_peer:
            sent(wq.at[0:n_peer], 1)
            sent(sqbuf.at[0:n_peer], 2)
            sent(qsend.at[0:n_peer], 3)
            sent(qsend.at[0:n_peer], 4)
            sent(wo.at[0 : n_peer * width], 8)
        if n_mate:
            sent(qmate.at[:, 0:n_mate], 5)
            sent(osend.at[:, 0:n_mate], 6)
            sent(ssend.at[:, 0:n_mate], 7)


def per_device(n_blk, n_tp, dec_states, norm_gain, query_weight, out_weight, enc_keys, enc_values):
    rows, feat = dec_states.shape
    width = query_weight.shape[1]
    enc_rows = enc_keys.shape[0]
    heads = width // HEAD_DIM
    n_pair = n_blk // 8
    bf16, f32 = jnp.bfloat16, jnp.float32
    dma = pltpu.SemaphoreType.DMA
    anywhere = pl.BlockSpec(memory_space=pl.ANY)
    return pl.pallas_call(
        functools.partial(kernel, n_blk, n_tp),
        out_shape=pltpu.VMEM((rows, feat), bf16),
        in_specs=[
            anywhere,
            anywhere,
            anywhere,
            anywhere,
            anywhere,
            anywhere,
        ],
        out_specs=pl.BlockSpec(memory_space=pltpu.VMEM),
        scratch_shapes=[
            pltpu.VMEM((1, n_tp * feat), f32),
            pltpu.VMEM((2 * heads, 8, enc_rows, HEAD_DIM), bf16),
            pltpu.VMEM((feat, width), bf16),
            pltpu.VMEM((n_tp, heads, feat, HEAD_DIM), bf16),
            pltpu.VMEM((n_tp * width, feat), bf16),
            pltpu.VMEM((rows, feat), bf16),
            pltpu.VMEM((rows, feat), bf16),
            pltpu.VMEM((n_tp, heads, rows, HEAD_DIM), bf16),
            pltpu.VMEM((n_tp, heads, rows, HEAD_DIM), bf16),
            pltpu.VMEM((rows, width), f32),
            pltpu.VMEM((n_tp, 8, rows), f32),
            pltpu.VMEM((rows, LANES), f32),
            pltpu.VMEM((heads, rows, HEAD_DIM), bf16),
            pltpu.VMEM((heads, n_pair, rows, HEAD_DIM), bf16),
            pltpu.VMEM((heads, n_pair, rows, HEAD_DIM), bf16),
            pltpu.VMEM((heads, n_pair, rows, HEAD_DIM), bf16),
            pltpu.VMEM((heads, n_pair, 1, rows), f32),
            pltpu.VMEM((heads, n_pair, 1, rows), f32),
            pltpu.VMEM((heads, rows, HEAD_DIM), f32),
            pltpu.VMEM((heads, rows, LANES), f32),
            pltpu.VMEM((rows, n_tp * width), bf16),
            pltpu.VMEM((rows, feat), f32),
            dma((9,)),
            dma((2 * heads, 3)),
            dma((heads,)),
            dma((n_tp - 1, heads, 2 * SUBS)),
            dma((n_tp - 1, heads)),
            dma((n_tp - 1,)),
            dma((2, n_tp - 1, heads + 1)),
            dma((3, heads + 1, max(n_pair - 1, 1))),
            dma((heads,)),
            dma((4,)),
        ],
        compiler_params=pltpu.CompilerParams(
            collective_id=0, has_side_effects=True, vmem_limit_bytes=60 * 1024 * 1024
        ),
    )(dec_states, norm_gain.reshape(1, -1), query_weight, out_weight, enc_keys, enc_values)


def solution(mesh):
    in_specs = (P("blk", "tp"), P(), P(None, "tp"), P("tp", None), P("blk", "tp"), P("blk", "tp"))
    out_specs = P("blk", "tp")
    body = functools.partial(per_device, mesh.shape["blk"], mesh.shape["tp"])
    return jax.shard_map(body, mesh=mesh, in_specs=in_specs, out_specs=out_specs, check_vma=False)
```

```python
import functools
import math

import jax
import jax.numpy as jnp
from jax import lax
from jax.experimental import pallas as pl
from jax.experimental.pallas import tpu as pltpu
from jax.sharding import PartitionSpec as P

HEAD_DIM = 128
NORM_EPS = 1e-06
LANES = 128
SUBS = 2


def column_tile(width, limit=640):
    best = LANES
    for tile in range(LANES, limit + 1, LANES):
        if width % tile == 0:
            best = tile
    return best


def kernel(
    n_blk,
    n_tp,
    x_hbm,
    gain_hbm,
    wq_hbm,
    wo_hbm,
    k_hbm,
    v_hbm,
    out_ref,
    gain_ref,
    kvbuf,
    wq_own,
    wq,
    wo,
    xbuf,
    xg,
    qsend,
    qrecv,
    own_part,
    sqbuf,
    fbuf,
    qbuf,
    qmate,
    osend,
    orecv,
    ssend,
    srecv,
    opart,
    lse_own,
    att,
    oacc,
    send_sem,
    kv_recv,
    kv_core_recv,
    wq_recv,
    wq_core_recv,
    sq_recv,
    head_recv,
    mate_recv,
    kv_local,
    local_sem,
):
    n_line = n_blk // 4
    n_pair = n_line // 2
    b = lax.axis_index("blk")
    t = lax.axis_index("tp")
    core = lax.rem(b, 2)
    side = lax.rem(lax.div(b, 2), 2)
    line = lax.div(b, 4)
    par = lax.rem(line, 2)
    pair = lax.div(line, 2)
    rows = x_hbm.shape[0]
    feat = x_hbm.shape[1]
    width = wq_hbm.shape[1]
    heads = width // HEAD_DIM
    span = n_tp * HEAD_DIM
    last = heads - 1
    wq_rows = feat // (4 * SUBS)
    wo_rows = HEAD_DIM // (4 * SUBS)

    def index(zz, yy, cc):
        return (zz * 2 + yy) * 2 + cc

    sibling = index(line, side, 1 - core)
    beside = index(line, 1 - side, core)
    partner = index(line + 1 - 2 * par, side, core)
    peers = [lax.rem(t + off, n_tp) for off in range(1, n_tp)]
    mates = [lax.rem(pair + off, n_pair) for off in range(1, n_pair)]
    n_peer, n_mate = len(peers), len(mates)

    def mate_index(m):
        return index(2 * m + par, side, core)

    def parts_of(h):
        if h < last:
            return [(h, slice(0, rows))]
        return [(h, slice(0, rows // 2)), (h + 1, slice(rows // 2, rows))]

    def ds(start, size, mult=LANES):
        return pl.ds(pl.multiple_of(start, mult), size)

    def head_cols(h):
        return slice(h * HEAD_DIM, (h + 1) * HEAD_DIM)

    def slot(pp, yy, cc):
        return (pp * 2 + yy) * 2 + cc

    mine = slot(par, side, core)

    kv_loads = [
        pltpu.make_async_copy(
            (k_hbm, v_hbm)[e % 2].at[:, head_cols(e // 2)], kvbuf.at[e, mine], kv_local.at[e // 2]
        )
        for e in range(2 * heads)
    ]
    x_load = pltpu.make_async_copy(x_hbm, xbuf, local_sem.at[0])
    gain_load = pltpu.make_async_copy(gain_hbm, gain_ref, local_sem.at[3])
    wq_load = pltpu.make_async_copy(wq_hbm.at[ds(t * feat, feat)], wq_own, local_sem.at[1])
    wo_loads = [
        pltpu.make_async_copy(
            wo_hbm.at[head_cols(h), ds(t * feat, feat)],
            wo.at[ds(h * span + t * HEAD_DIM, HEAD_DIM)],
            local_sem.at[2],
        )
        for h in range(heads)
    ]
    for load in kv_loads[:2] + [gain_load, x_load, wq_load] + kv_loads[2:] + wo_loads:
        load.start()

    barrier = pltpu.get_barrier_semaphore()
    for other in [sibling, beside, partner] + [mate_index(m) for m in mates]:
        pl.semaphore_signal(barrier, inc=1, device_id={"blk": other})
    for p in peers:
        pl.semaphore_signal(barrier, inc=1, device_id={"tp": p})
    pl.semaphore_wait(barrier, 3 + len(mates) + len(peers))

    def remote(src, dst, kind, recv_sem, device_id):
        return pltpu.make_async_remote_copy(
            src_ref=src,
            dst_ref=dst,
            send_sem=send_sem.at[kind],
            recv_sem=recv_sem,
            device_id=device_id,
        )

    def arrived(ref, recv_sem):
        remote(ref, ref, 0, recv_sem, {"blk": sibling}).wait_recv()

    def sent(ref, kind):
        remote(ref, ref, kind, kv_core_recv.at[0], {"blk": sibling}).wait_send()

    def kv_send(e, s, kind, target):
        ref = kvbuf.at[e, s]
        remote(ref, ref, 0, kv_recv.at[e, kind], {"blk": target}).start()

    def kv_share(e, s):
        ref = kvbuf.at[e, s]
        remote(ref, ref, 0, kv_core_recv.at[e // 2], {"blk": sibling}).start()

    def kv_wait(e, s, kind):
        arrived(kvbuf.at[e, s], kv_recv.at[e, kind])

    from_beside = slot(par, 1 - side, core)
    from_partner = slot(1 - par, side, core)
    from_corner = slot(1 - par, 1 - side, core)

    def kv_loaded(h):
        both = kvbuf.at[2 * h : 2 * h + 2, mine]
        pltpu.make_async_copy(both, both, kv_local.at[h]).wait()

    def kv_line(e):
        kv_send(e, mine, 1, partner)

    def kv_side(e):
        kv_send(e, mine, 0, beside)

    def kv_core(e):
        kv_share(e, mine)

    def kv_from_partner(e):
        kv_wait(e, from_partner, 1)
        kv_send(e, from_partner, 2, beside)
        kv_share(e, from_partner)

    def kv_from_beside(e):
        kv_wait(e, from_beside, 0)
        kv_share(e, from_beside)

    def kv_from_corner(e):
        kv_wait(e, from_corner, 2)
        kv_share(e, from_corner)

    def kv_ready(h):
        arrived(kvbuf.at[2 * h : 2 * h + 2, 0:4], kv_core_recv.at[h])

    def wq_chunk(pp, cc, sub):
        return (pp * 2 + cc) * SUBS + sub

    def wq_ref(p, h, c):
        return wq.at[p, h, ds(c * wq_rows, wq_rows, 16)]

    def wq_hop(j, h, c, k):
        ref = wq_ref(peers[j], h, c)
        remote(ref, ref, 1, wq_recv.at[j, h, k], {"blk": partner}).start()

    def wq_share(j, h, c):
        ref = wq_ref(peers[j], h, c)
        remote(ref, ref, 1, wq_core_recv.at[j, h], {"blk": sibling}).start()

    def wq_start(h, k):
        for j, p in enumerate(peers):
            c = wq_chunk(par if k < SUBS else 1 - par, core, k % SUBS)
            src = wq_hbm.at[ds(p * feat + c * wq_rows, wq_rows, 16), head_cols(h)]
            place = wq_recv.at[n_peer - 1 - j, h, k]
            remote(src, wq_ref(t, h, c), 1, place, {"tp": p}).start()

    def wq_pass(h, sub):
        for j, p in enumerate(peers):
            c = wq_chunk(par, core, sub)
            arrived(wq_ref(p, h, c), wq_recv.at[j, h, sub])
            if h != last:
                wq_hop(j, h, c, SUBS + sub)
            wq_share(j, h, c)

    def wq_relay(h, sub):
        for j, p in enumerate(peers):
            c = wq_chunk(1 - par, core, sub)
            arrived(wq_ref(p, h, c), wq_recv.at[j, h, SUBS + sub])
            wq_share(j, h, c)

    def q_part(h):
        for j, p in enumerate(peers):
            arrived(wq.at[p, h, 0 : feat // 2], wq_core_recv.at[j, h])
            qsend[p, h] = jnp.dot(
                xg[...], wq[p, h], preferred_element_type=jnp.float32
            ).astype(jnp.bfloat16)
            for place, part in parts_of(h):
                remote(
                    qsend.at[p, h, part],
                    qrecv.at[t, h, part],
                    3,
                    head_recv.at[n_peer - 1 - j, place],
                    {"tp": p},
                ).start()

    tile = column_tile(feat)

    def norm():
        gain_load.wait()
        x_load.wait()
        squares = jnp.zeros((rows, 1), jnp.float32)
        for start in range(0, feat, tile):
            piece = xbuf[:, start : start + tile].astype(jnp.float32)
            squares += jnp.sum(piece * piece, axis=1, keepdims=True)
            gain = gain_ref[:, ds(t * feat + start, tile)]
            xg[:, start : start + tile] = (piece * gain).astype(jnp.bfloat16)
        wide = jnp.broadcast_to(squares, (rows, LANES))
        sqbuf[t] = jnp.transpose(wide)[0:8, :]
        for j, p in enumerate(peers):
            ref = sqbuf.at[t]
            remote(ref, ref, 2, sq_recv.at[n_peer - 1 - j], {"tp": p}).start()
        wq_load.wait()
        own_part[...] = jnp.dot(xg[...], wq_own[...], preferred_element_type=jnp.float32)

    def factor():
        total = sqbuf[t][0:1, :]
        for j, p in enumerate(peers):
            arrived(sqbuf.at[p], sq_recv.at[j])
            total = total + sqbuf[p][0:1, :]
        column = jnp.transpose(jnp.broadcast_to(total, (LANES, rows)))
        scale = math.log2(math.e) / math.sqrt(HEAD_DIM)
        fbuf[...] = lax.rsqrt(column / (feat * n_tp) + NORM_EPS) * scale

    def mate_send(k, src, dst, place, i):
        there = mate_recv.at[k, place, n_mate - 1 - i]
        remote(src, dst, 5 + k, there, {"blk": mate_index(mates[i])}).start()

    def q_make(h, b):
        place, part = parts_of(h)[b]
        summed = own_part[part, head_cols(h)]
        for j, p in enumerate(peers):
            arrived(qrecv.at[p, h, part], head_recv.at[j, place])
            summed = summed + qrecv[p, h, part].astype(jnp.float32)
        qbuf[h, part] = (summed * fbuf[part]).astype(jnp.bfloat16)
        for i in range(n_mate):
            mate_send(0, qbuf.at[h, part], qmate.at[h, pair, part], place, i)

    def attend(h, query, emit):
        half = rows // 2

        def score(b):
            block = query(b, slice(b * half, b * half + half))
            scores = []
            for i in range(4):
                keys = kvbuf[2 * h, 2 * i : 2 * i + 2].reshape(-1, HEAD_DIM)
                scores.append(
                    lax.dot_general(
                        block, keys, (((1,), (1,)), ((), ())), preferred_element_type=jnp.float32
                    )
                )
            return scores

        later = score(0)
        for b in range(2):
            scores = later
            if b == 0:
                later = score(1)
            top = scores[0]
            for s in scores[1:]:
                top = jnp.maximum(top, s)
            top = jnp.max(top, axis=1, keepdims=True)
            mixed = jnp.zeros((half, 2 * HEAD_DIM), jnp.float32)
            for i in range(4):
                vals = kvbuf[2 * h + 1, 2 * i : 2 * i + 2].reshape(-1, HEAD_DIM)
                wide = jnp.concatenate([vals, jnp.ones_like(vals)], axis=1)
                weights = jnp.exp2(scores[i] - top).astype(jnp.bfloat16)
                mixed = mixed + jnp.dot(weights, wide, preferred_element_type=jnp.float32)
            total = mixed[:, HEAD_DIM:]
            lse = top + jnp.log(total) * math.log2(math.e)
            emit(b, slice(b * half, b * half + half), mixed[:, :HEAD_DIM] / total, lse)

    def att_own(h):
        def emit(b, part, out, lse):
            opart[h, part] = out
            lse_own[h, part] = lse

        attend(h, lambda b, part: qbuf[h, part], emit)

    def o_send(h, b):
        place, part = parts_of(h)[b]
        for i, m in enumerate(mates):
            mate_send(1, osend.at[h, m, part], orecv.at[h, pair, part], place, i)
            here, there = ssend.at[h, m, :, part], srecv.at[h, pair, :, part]
            mate_send(2, here, there, place, i)

    def att_mate(h):
        for i, m in enumerate(mates):

            def query(b, part):
                if b < len(parts_of(h)):
                    place, piece = parts_of(h)[b]
                    arrived(qmate.at[h, m, piece], mate_recv.at[0, place, i])
                return qmate[h, m, part]

            def emit(b, part, out, lse):
                osend[h, m, part] = out.astype(jnp.bfloat16)
                ssend[h, m, :, part] = jnp.transpose(lse)[0:1, :]

            attend(h, query, emit)

    def att_ref(p, h, part):
        return att.at[part, ds(h * span + p * HEAD_DIM, HEAD_DIM)]

    def merge(h, b):
        place, part = parts_of(h)[b]
        parts = [opart[h, part]]
        logs = [lse_own[h, part]]
        for i, m in enumerate(mates):
            arrived(srecv.at[h, m, :, part], mate_recv.at[2, place, i])
            arrived(orecv.at[h, m, part], mate_recv.at[1, place, i])
            parts.append(orecv[h, m, part].astype(jnp.float32))
            stat = srecv[h, m, :, part]
            logs.append(jnp.transpose(jnp.broadcast_to(stat, (LANES, stat.shape[1]))))
        top = logs[0]
        for log in logs[1:]:
            top = jnp.maximum(top, log)
        shares = [jnp.exp2(log - top) for log in logs]
        total = shares[0]
        mixed = shares[0] * parts[0]
        for share, piece in zip(shares[1:], parts[1:]):
            total = total + share
            mixed = mixed + share * piece
        att[part, ds(h * span + t * HEAD_DIM, HEAD_DIM)] = (mixed / total).astype(jnp.bfloat16)
        for j, p in enumerate(peers):
            there = head_recv.at[n_peer - 1 - j, place]
            remote(att_ref(t, h, part), att_ref(t, h, part), 4, there, {"tp": p}).start()

    def att_wait(h, b):
        place, part = parts_of(h)[b]
        for j, p in enumerate(peers):
            arrived(att_ref(p, h, part), head_recv.at[j, place])

    def wo_ref(p, h, q):
        return wo.at[ds(h * span + p * HEAD_DIM + q * wo_rows, wo_rows, wo_rows)]

    def wo_chunk(yy, cc, sub):
        return (yy * 2 + cc) * SUBS + sub

    def wo_start(h, k):
        q = wo_chunk(side if k < SUBS else 1 - side, core, k % SUBS)
        for j, p in enumerate(peers):
            src = wo_hbm.at[ds(h * HEAD_DIM + q * wo_rows, wo_rows, wo_rows), ds(p * feat, feat)]
            place = wq_recv.at[n_peer - 1 - j, h, k]
            remote(src, wo_ref(t, h, q), 8, place, {"tp": p}).start()

    def wo_pass(h, sub):
        for j, p in enumerate(peers):
            ref = wo_ref(p, h, wo_chunk(side, core, sub))
            arrived(ref, wq_recv.at[j, h, sub])
            if h != last or sub == 0:
                remote(ref, ref, 8, wq_recv.at[j, h, SUBS + sub], {"blk": beside}).start()
            remote(ref, ref, 8, wq_core_recv.at[j, h], {"blk": sibling}).start()

    def wo_relay(h, sub):
        for j, p in enumerate(peers):
            ref = wo_ref(p, h, wo_chunk(1 - side, core, sub))
            arrived(ref, wq_recv.at[j, h, SUBS + sub])
            remote(ref, ref, 8, wq_core_recv.at[j, h], {"blk": sibling}).start()

    def wo_loaded():
        ref = wo.at[0:width]
        pltpu.make_async_copy(ref, ref, local_sem.at[2]).wait()

    def wo_ready(h):
        for j in range(n_peer):
            arrived(wo.at[0 : HEAD_DIM // 2], wq_core_recv.at[j, h])

    starts = range(0, feat, tile)

    def project(h):
        if h == 0:
            wo_loaded()
        wo_ready(h)
        att_wait(h, 0)
        for start in starts:
            cols = slice(start, start + tile)
            block = slice(h * span, (h + 1) * span)
            result = jnp.dot(att[:, block], wo[block, cols], preferred_element_type=jnp.float32)
            oacc[:, cols] = result if h == 0 else oacc[:, cols] + result

    events = []

    def at(when, step, *args):
        events.append((when, len(events), step, args))

    for h in range(heads):
        k, v = 2 * h, 2 * h + 1
        stage = max(h - last + 2, 0)
        for piece in range(2 * SUBS if h == last else SUBS):
            at(12.01 if piece >= 2 * SUBS - 1 else 2.0 + 0.1 * h, wq_start, h, piece)
        at(2.45 if h == 0 else 2.6 + 0.01 * h, kv_loaded, h)
        for e in (k, v):
            at((2.5 + 0.01 * e, 9.36, 14.25 if e == k else 16.55)[stage], kv_line, e)
            at((2.5 + 0.01 * e, 2.65, 7.05)[stage], kv_side, e)
            at(2.7 + 0.01 * e, kv_core, e)
        at((4.9, 16.2, 21.85)[stage], kv_from_partner, k)
        at((7.0, 18.1, 24.6)[stage], kv_from_partner, v)
        at((7.1, 9.4, 20.2)[stage], kv_from_beside, k)
        at((7.2, 10.8, 20.3)[stage], kv_from_beside, v)
        at((12.6, 22.6, 27.1)[stage], kv_from_corner, k)
        at((14.6, 24.7, 28.2)[stage], kv_from_corner, v)
        for piece in range(2 * SUBS if h == last else SUBS):
            if piece != SUBS:
                at((16.05, 20.2, 23.65)[stage], wo_start, h, piece)
        for sub in range(SUBS):
            at((4.2, 7.6, 11.2)[stage] + 1.75 * sub, wq_pass, h, sub)
            at((10.2, 14.2, 15.2)[stage] + (3.3 if h == last else 0.1) * sub, wq_relay, h, sub)
            at(((25.0, 26.15), (28.25, 28.3), (30.43, 30.6))[stage][sub], wo_pass, h, sub)
            at((30.9, 34.03, 34.2)[stage], wo_relay, h, sub)
        at((12.0, 16.0, 20.0)[stage], q_part, h)
        at((15.5, 20.1, 23.5)[stage], q_make, h, 0)
        at((16.6, 25.9, 30.2)[stage], kv_ready, h)
        at((16.7, 26.1, 30.5)[stage], att_own, h)
        at((21.9, 27.2, 30.4)[stage], att_mate, h)
        if h < last:
            at(34.05 if h < last - 1 else 37.5, project, h)
        for b in range(len(parts_of(h))):
            at((24.5, 27.25, 30.4)[stage], o_send, h, b)
        at((31.0, 31.9, 33.2)[stage], merge, h, 0)
    at(23.6, q_make, last, 1)
    at(34.0, merge, last, 1)
    at(4.0, norm)
    at(15.45, factor)
    for when, order, step, args in sorted(events, key=lambda event: event[:2]):
        with jax.named_scope("_".join([step.__name__] + [str(a) for a in args])):
            step(*args)

    wo_ready(last)
    with jax.named_scope("drain"):
        sent(kvbuf.at[:, 0:7], 0)
        if n_peer:
            sent(wq.at[0:n_peer], 1)
            sent(sqbuf.at[0:n_peer], 2)
            sent(qsend.at[0:n_peer], 3)
            sent(wo.at[0 : n_peer * width], 8)
        if n_mate:
            sent(qmate.at[:, 0:n_mate], 5)
            sent(osend.at[:, 0:n_mate], 6)
            sent(ssend.at[:, 0:n_mate], 7)
    for b, (place, part) in enumerate(parts_of(last)):
        with jax.named_scope(f"tail_wait_{b}"):
            att_wait(last, b)
        for start in starts:
            cols = slice(start, start + tile)
            result = oacc[part, cols] + jnp.dot(
                att[part, last * span :],
                wo[last * span :, cols],
                preferred_element_type=jnp.float32,
            )
            out_ref[part, cols] = result.astype(jnp.bfloat16)
    if n_peer:
        sent(qsend.at[0:n_peer], 4)


def per_device(n_blk, n_tp, dec_states, norm_gain, query_weight, out_weight, enc_keys, enc_values):
    rows, feat = dec_states.shape
    width = query_weight.shape[1]
    enc_rows = enc_keys.shape[0]
    heads = width // HEAD_DIM
    n_pair = n_blk // 8
    bf16, f32 = jnp.bfloat16, jnp.float32
    dma = pltpu.SemaphoreType.DMA
    anywhere = pl.BlockSpec(memory_space=pl.ANY)
    return pl.pallas_call(
        functools.partial(kernel, n_blk, n_tp),
        out_shape=pltpu.VMEM((rows, feat), bf16),
        in_specs=[
            anywhere,
            anywhere,
            anywhere,
            anywhere,
            anywhere,
            anywhere,
        ],
        out_specs=pl.BlockSpec(memory_space=pltpu.VMEM),
        scratch_shapes=[
            pltpu.VMEM((1, n_tp * feat), f32),
            pltpu.VMEM((2 * heads, 8, enc_rows, HEAD_DIM), bf16),
            pltpu.VMEM((feat, width), bf16),
            pltpu.VMEM((n_tp, heads, feat, HEAD_DIM), bf16),
            pltpu.VMEM((n_tp * width, feat), bf16),
            pltpu.VMEM((rows, feat), bf16),
            pltpu.VMEM((rows, feat), bf16),
            pltpu.VMEM((n_tp, heads, rows, HEAD_DIM), bf16),
            pltpu.VMEM((n_tp, heads, rows, HEAD_DIM), bf16),
            pltpu.VMEM((rows, width), f32),
            pltpu.VMEM((n_tp, 8, rows), f32),
            pltpu.VMEM((rows, LANES), f32),
            pltpu.VMEM((heads, rows, HEAD_DIM), bf16),
            pltpu.VMEM((heads, n_pair, rows, HEAD_DIM), bf16),
            pltpu.VMEM((heads, n_pair, rows, HEAD_DIM), bf16),
            pltpu.VMEM((heads, n_pair, rows, HEAD_DIM), bf16),
            pltpu.VMEM((heads, n_pair, 1, rows), f32),
            pltpu.VMEM((heads, n_pair, 1, rows), f32),
            pltpu.VMEM((heads, rows, HEAD_DIM), f32),
            pltpu.VMEM((heads, rows, LANES), f32),
            pltpu.VMEM((rows, n_tp * width), bf16),
            pltpu.VMEM((rows, feat), f32),
            dma((9,)),
            dma((2 * heads, 3)),
            dma((heads,)),
            dma((n_tp - 1, heads, 2 * SUBS)),
            dma((n_tp - 1, heads)),
            dma((n_tp - 1,)),
            dma((n_tp - 1, heads + 1)),
            dma((3, heads + 1, max(n_pair - 1, 1))),
            dma((heads,)),
            dma((4,)),
        ],
        compiler_params=pltpu.CompilerParams(
            collective_id=0, has_side_effects=True, vmem_limit_bytes=60 * 1024 * 1024
        ),
    )(dec_states, norm_gain.reshape(1, -1), query_weight, out_weight, enc_keys, enc_values)


def solution(mesh):
    in_specs = (P("blk", "tp"), P(), P(None, "tp"), P("tp", None), P("blk", "tp"), P("blk", "tp"))
    out_specs = P("blk", "tp")
    body = functools.partial(per_device, mesh.shape["blk"], mesh.shape["tp"])
    return jax.shard_map(body, mesh=mesh, in_specs=in_specs, out_specs=out_specs, check_vma=False)
```
